512 devices in a mesh: groups: 2 (over y), docs: 16 (over z), mp: 8 (over x), sub: 2 (over core).
Axes of the slice: x: 8, y: 2, z: 16, core: 2. Of those that a mesh axis runs over, the one named last changes fastest.
The devices are a block of a 8x8x16 slice.
Arguments:
- embeddings: bfloat16 [65536, 1024], P(('groups', 'docs', 'mp', 'sub')), parts along dimension 0, may hold values from -6 to 6
- owner_shard: int32 [65536, 1], P(('groups', 'docs', 'mp', 'sub')), parts along dimension 0, may hold values from 0 to 15; in each aligned block of 128 rows (0 to 127, 128 to 255, ...) at most 16 rows name the same one
- query_local: int32 [65536], P(('groups', 'docs', 'mp', 'sub')), parts along dimension 0, may hold values from 0 to 1
- labels: int32 [65536], P(('groups', 'docs', 'mp', 'sub')), parts along dimension 0, may hold values from 0 to 4
- w_first: bfloat16 [1024, 1024], replicated, may hold values from -0.1875 to 0.1875
- w_second: float32 [1024], replicated, may hold values from -0.1875 to 0.1875
Outputs:
- emb_grad: bfloat16 [65536, 1024], P(('groups', 'docs', 'mp', 'sub')), parts along dimension 0
- w_first_grad: float32 [2048, 1024], P(('groups', 'mp', 'sub')), parts along dimension 0
- w_second_grad: float32 [2048], P('groups'), parts along dimension 0
The draws below stay inside these ranges and needn't reach their ends.
There are 2 independent parts, one for each index of `groups`. The reference program is written for one: setup_inputs(seed, part) draws one part's arguments, and reference() takes and returns one part's arrays. A program takes and returns all parts, laid end to end along the dimension named above; an argument that names none is the same for every part. Nothing has to cross between parts.
Inputs may be any that keep to these rules, and one draw needn't show every extreme that they name: `owner_shard`: among the 128 rows of one document shard no owner appears more than 16 times, and some owner appears exactly 16 times.
All inputs are finite; a program needn't handle non-finite values.
Results may differ from the reference program's by a relative error of at most 0.017.
Values may be sent and summed in bfloat16 or wider, within the bound.
No kernel may reach another device: no remote copies, remote signals or barrier semaphores. Data moves between devices by JAX's collectives and lax.ppermute only.
A program may use at most 64 MiB of HBM per device.

```python
import math
import jax
import jax.numpy as jnp
import numpy as np
from jax import lax

E = 1024
H = 1024
C_DEV = 128
Q_DEV = 2
CAND = 32768
CAP = 16
N_DOCS = 16
N_MP = 8
N_SUB = 2


def with_ends(entries, own_key, low, top_value):
    place = [jax.random.randint(jax.random.fold_in(own_key, axis), (), 0, length) for axis, length in enumerate(entries.shape)]
    main_axis = entries.shape.index(max(entries.shape))
    beside = place[:main_axis] + [(place[main_axis] + 1) % entries.shape[main_axis]] + place[main_axis + 1:]
    return entries.at[tuple(place)].set(low).at[tuple(beside)].set(top_value)


def shard_levels(own_key, dims, split, least, top_value):
    def one(axis_at, shards_of):
        heights = jax.random.uniform(jax.random.fold_in(jax.random.fold_in(own_key, 6), axis_at), (shards_of,), jnp.float32, least / len(split), top_value / len(split))
        return jnp.repeat(jnp.exp(heights), dims[axis_at] // shards_of).reshape((-1,) + (1,) * (len(dims) - axis_at - 1))

    loudness = one(*split[0])
    for cut in split[1:]:
        loudness = loudness * one(*cut)
    return loudness


def shared_out(key, own, number, rows, count, top, reach, lean):
    sequence = jax.random.permutation(key, count)
    packed, ordinary = shares(count, rows * top, reach, lean, True), shares(count, rows * top, reach, lean, False)
    places = jnp.arange(count)

    def named(tallies, offset_by):
        used = int((tallies > 0).sum())
        fixed = max(1, used // 4)
        shifted = fixed + (places - fixed + offset_by * (used - fixed)) % max(1, count - fixed)
        return jnp.zeros((count,), jnp.int32).at[sequence[jnp.where(places < fixed, places, shifted)]].set(jnp.asarray(tallies, jnp.int32))

    tallies = jnp.where(number % 4 == 0, named(packed, number // 4), named(ordinary, number - number // 4 - 1))
    mixed = jax.random.permutation(jax.random.fold_in(own, 3), count)
    giver, sink = mixed[0:count // 2 * 2:2], mixed[1:count // 2 * 2:2]
    margin = jnp.minimum(tallies[giver] - 1, reach - tallies[sink]) // 2
    margin = jnp.where((giver == sequence[0]) | (sink == sequence[0]) | (tallies[sink] == 0), 0, jnp.maximum(margin, 0))
    shifted = jax.random.randint(jax.random.fold_in(own, 4), (count // 2,), 0, 1 << 20) % (margin + 1)
    tallies = tallies.at[giver].add(-shifted).at[sink].add(shifted)
    items = jnp.searchsorted(jnp.cumsum(tallies), jnp.arange(rows * top), side="right").astype(jnp.int32)
    listing = items.reshape(top, rows).T
    listing = listing[jax.random.permutation(jax.random.fold_in(own, 1), rows)]
    offset_by = jax.random.randint(jax.random.fold_in(own, 2), (rows, 1), 0, top)
    return jnp.take_along_axis(listing, (jnp.arange(top)[None, :] + offset_by) % top, axis=1)


def shares(count, total, most, slope, full):
    portions = [(1 << 20) // math.isqrt(grade ** slope) + 1 for grade in range(1, count + 1)]
    largest = most if full else min(most, max(-(-total // count), total * portions[0] // sum(portions)))
    least = 1 if total - largest >= count - 1 else 0
    holding, rest = [largest] + [least] * (count - 1), total - largest - least * (count - 1)
    while rest > 0:
        movable = [i for i in range(1, count) if holding[i] < largest] or [i for i in range(1, count) if holding[i] < most]
        mass, left = sum([portions[i] for i in movable]), rest
        for i in movable:
            extra = min(most - holding[i], max(1, left * portions[i] // mass), rest)
            holding[i] = holding[i] + extra
            rest = rest - extra
    return np.array(holding)


def scatter_about(stream_key, extent, spread, most, pieces=(), held_as=jnp.bfloat16):
    result = jax.random.normal(stream_key, extent, jnp.float32) * spread
    if len(pieces) > 0:
        result = shard_levels(stream_key, extent, pieces, -0.22, 0.18) * result
    return jnp.clip(result, min=-most, max=most).astype(held_as)


def setup_inputs(seed: int = 0, part: int = 0) -> dict:
    streams_of = jax.random.split(jax.random.key(seed), 7)
    part_keys = jax.random.split(jax.random.fold_in(streams_of[6], part), 7)
    embeddings = scatter_about(part_keys[0], (CAND, E), 1.0, 6.0, ((0, 256),))
    owner_shard_keys = jax.random.split(jax.random.fold_in(part_keys[1], 1), CAND // C_DEV)
    owner_shard_turns = jax.random.permutation(jax.random.fold_in(part_keys[1], 3), CAND // C_DEV)
    owner_shard = jax.vmap(lambda own, number: shared_out(jax.random.fold_in(part_keys[1], 2), own, number, C_DEV, N_DOCS, 1, CAP, 2))(owner_shard_keys, owner_shard_turns).reshape((CAND, 1))
    query_local = with_ends(jax.random.randint(part_keys[2], (CAND,), 0, Q_DEV), jax.random.fold_in(part_keys[2], 1), 0, Q_DEV - 1).astype(jnp.int32)
    labels = with_ends(jax.random.randint(part_keys[3], (CAND,), 0, 5), jax.random.fold_in(part_keys[3], 1), 0, 4).astype(jnp.int32)
    w_first = scatter_about(streams_of[4], (E, H), E ** -0.5, 0.1875)
    w_second = scatter_about(streams_of[5], (H,), H ** -0.5, 0.1875, (), jnp.float32)
    return {"embeddings": embeddings, "owner_shard": owner_shard, "query_local": query_local, "labels": labels, "w_first": w_first, "w_second": w_second}


ranking_softness = 1.0


def silu_slope(pre_act):
    sigmoid_v = jax.nn.sigmoid(pre_act)
    return sigmoid_v * (1.0 + pre_act * (1.0 - sigmoid_v))


def rank_rows(row_start, row_count, scorer_outputs, query_mark, grade_slot):
    row_query = lax.dynamic_slice_in_dim(query_mark, row_start, row_count)
    single_row_score = lax.dynamic_slice_in_dim(scorer_outputs, row_start, row_count)
    row_label = lax.dynamic_slice_in_dim(grade_slot, row_start, row_count)
    slot_index = jnp.arange(scorer_outputs.shape[0], dtype=jnp.int32)
    row_index = row_start + jnp.arange(row_count, dtype=jnp.int32)
    matching_query = (row_query[:, None] == query_mark[None, :]) & (row_query[:, None] > 0)
    smooth_rank = jnp.sum(jnp.where(matching_query, jax.nn.sigmoid((scorer_outputs[None, :] - single_row_score[:, None]) / ranking_softness), 0.0), axis=1) - 0.5
    higher = (grade_slot[None, :] > row_label[:, None]) | ((grade_slot[None, :] == row_label[:, None]) & (slot_index[None, :] < row_index[:, None]))
    ideal_rank = jnp.sum((matching_query & higher).astype(jnp.float32), axis=1)
    row_gain = jnp.exp2(row_label.astype(jnp.float32)) - 1.0
    return smooth_rank, row_gain / jnp.log2(2.0 + ideal_rank)


def lambda_rows(row_start, row_count, scorer_outputs, query_mark, grade_slot, discount, inv_ideal):
    gain_all = jnp.exp2(grade_slot.astype(jnp.float32)) - 1.0
    row_query = lax.dynamic_slice_in_dim(query_mark, row_start, row_count)
    single_row_score = lax.dynamic_slice_in_dim(scorer_outputs, row_start, row_count)
    row_label = lax.dynamic_slice_in_dim(grade_slot, row_start, row_count)
    row_gain = lax.dynamic_slice_in_dim(gain_all, row_start, row_count)
    row_disc = lax.dynamic_slice_in_dim(discount, row_start, row_count)
    row_inv = lax.dynamic_slice_in_dim(inv_ideal, row_start, row_count)
    matching_query = (row_query[:, None] == query_mark[None, :]) & (row_query[:, None] > 0)
    score_gap = single_row_score[:, None] - scorer_outputs[None, :]
    weights = jnp.abs(row_gain[:, None] - gain_all[None, :]) * jnp.abs(row_disc[:, None] - discount[None, :]) * row_inv[:, None]
    direction = jnp.where(row_label[:, None] > grade_slot[None, :], -jax.nn.sigmoid(-score_gap), 0.0) + jnp.where(grade_slot[None, :] > row_label[:, None], jax.nn.sigmoid(score_gap), 0.0)
    return jnp.sum(jnp.where(matching_query, weights * direction, 0.0), axis=1)


def owner_lambdas(scorer_outputs, query_mark, grade_slot):
    slot_total = scorer_outputs.shape[0]
    row_count = math.gcd(slot_total, 512)
    starts = jnp.arange(0, slot_total, row_count, dtype=jnp.int32)

    def rank_block(first_row):
        return rank_rows(first_row, row_count, scorer_outputs, query_mark, grade_slot)

    smooth_rank, ideal_term = lax.map(rank_block, starts)
    smooth_rank = smooth_rank.reshape(slot_total)
    ideal_term = ideal_term.reshape(slot_total)
    discount = 1.0 / jnp.log2(2.0 + smooth_rank)
    member = (query_mark[:, None] == jnp.arange(1, Q_DEV + 1, dtype=jnp.int32)[None, :]).astype(jnp.float32)
    per_query = jnp.dot(ideal_term, member, precision=lax.Precision.HIGHEST)
    idcg = jnp.dot(member, per_query, precision=lax.Precision.HIGHEST)
    inv_ideal = jnp.where(idcg > 0.0, 1.0 / jnp.where(idcg > 0.0, idcg, 1.0), 0.0)

    def lambda_block(first_row):
        return lambda_rows(first_row, row_count, scorer_outputs, query_mark, grade_slot, discount, inv_ideal)

    return lax.map(lambda_block, starts).reshape(slot_total)


def owner_step(triple):
    return owner_lambdas(triple[0], triple[1], triple[2])


def reference(embeddings, owner_shard, query_local, labels, w_first, w_second):
    lanes = N_MP * N_SUB
    shards = N_DOCS * lanes
    slot_total = N_DOCS * CAP
    whole = shards * slot_total
    target = owner_shard[:, 0].astype(jnp.int32)
    hits = (target.reshape(shards, C_DEV)[:, :, None] == jnp.arange(N_DOCS, dtype=jnp.int32)[None, None, :]).astype(jnp.int32)
    before = (jnp.cumsum(hits, axis=1).astype(jnp.int32) - hits) * hits
    earlier = jnp.sum(before, axis=2).astype(jnp.int32).reshape(CAND)
    block_of = jnp.arange(CAND, dtype=jnp.int32) // C_DEV
    lane_of = block_of % lanes
    source_of = block_of // lanes
    slot_of = (((lane_of * N_DOCS + target) * N_DOCS + source_of) * CAP + earlier).astype(jnp.int32)
    emb_blocks = embeddings.reshape(shards, C_DEV, E)

    def forward(block):
        pre_act = jnp.dot(block, w_first, preferred_element_type=jnp.float32)
        hidden = pre_act * jax.nn.sigmoid(pre_act)
        return jnp.dot(hidden, w_second, precision=lax.Precision.HIGHEST)

    scorer_outputs = lax.map(forward, emb_blocks).reshape(CAND)
    query_mark = jnp.zeros((whole,), jnp.int32).at[slot_of].set(query_local.astype(jnp.int32) + 1)
    grade_slot = jnp.zeros((whole,), jnp.int32).at[slot_of].set(labels.astype(jnp.int32))
    score_slot = jnp.zeros((whole,), jnp.float32).at[slot_of].set(scorer_outputs)
    lambda_slot = lax.map(owner_step, (score_slot.reshape(shards, slot_total), query_mark.reshape(shards, slot_total), grade_slot.reshape(shards, slot_total)))
    lambdas = lambda_slot.reshape(whole)[slot_of]
    lambda_blocks = lambdas.reshape(shards, C_DEV)

    def backward(carry, pair):
        block, lambda_per_block = pair
        pre_act = jnp.dot(block, w_first, preferred_element_type=jnp.float32)
        hidden = pre_act * jax.nn.sigmoid(pre_act)
        pre_grad = (lambda_per_block[:, None] * w_second[None, :] * silu_slope(pre_act)).astype(jnp.bfloat16)
        emb_part = lax.dot_general(pre_grad, w_first, (((1,), (1,)), ((), ())), preferred_element_type=jnp.float32).astype(jnp.bfloat16)
        first = carry[0] + lax.dot_general(block, pre_grad, (((0,), (0,)), ((), ())), preferred_element_type=jnp.float32)
        second = carry[1] + jnp.dot(lambda_per_block, hidden, precision=lax.Precision.HIGHEST)
        return (first, second), emb_part

    start_carry = (jnp.zeros((E, H), jnp.float32), jnp.zeros((H,), jnp.float32))
    totals, emb_parts = lax.scan(backward, start_carry, (emb_blocks, lambda_blocks))
    return emb_parts.reshape(CAND, E), totals[0], totals[1]
```

```python
import functools

import jax
import jax.numpy as jnp
from jax import lax
from jax.experimental import pallas as pl
from jax.experimental.pallas import tpu as pltpu
from jax.sharding import PartitionSpec as P

LANES = 128


def whole(*shape_and_type):
    return jax.ShapeDtypeStruct(*shape_and_type)


def vmem_specs(count):
    return [pl.BlockSpec(memory_space=pltpu.VMEM)] * count


def score_kernel(capacity, emb_ref, w1_ref, w2_ref, owner_ref, query_ref, label_ref, sent_ref, pre_ref, slot_ref):
    rows = emb_ref.shape[0]
    halves = sent_ref.shape[0] // 4
    along = lax.broadcasted_iota(jnp.int32, (rows, rows), 1)
    down = lax.broadcasted_iota(jnp.int32, (rows, rows), 0)

    def column(row):
        return jnp.sum(jnp.where(along == down, row, 0), axis=1, keepdims=True)

    owner = owner_ref[...]
    owner_column = column(owner)
    earlier = jnp.where((owner_column == owner) & (along < down), 1, 0)
    slot = owner_column * capacity + jnp.sum(earlier, axis=1, keepdims=True)
    slot_ref[...] = slot
    mark = column(query_ref[...] + 1).astype(jnp.float32)
    label = column(label_ref[...]).astype(jnp.float32)

    pre_act = jnp.dot(emb_ref[...], w1_ref[...], preferred_element_type=jnp.float32)
    pre_ref[...] = pre_act
    hidden = pre_act * jax.nn.sigmoid(pre_act)
    score = jnp.sum(hidden * w2_ref[...], axis=1, keepdims=True)

    lane = lax.broadcasted_iota(jnp.int32, (rows, LANES), 1)
    sent_ref[...] = jnp.zeros_like(sent_ref)
    for h in range(halves):
        here = slot == lane + h * LANES
        for place, value in enumerate((score, mark, label)):
            sent_ref[place * halves + h : place * halves + h + 1, :] = jnp.sum(
                jnp.where(here, value, 0.0), axis=0, keepdims=True
            )


def within_groups(x, capacity):
    lane = lax.broadcasted_iota(jnp.int32, x.shape, 1)
    out = [x]
    step = capacity // 2
    while step:
        upper = (lane & step) != 0
        spread = []
        for y in out:
            spread.append(jnp.where(upper, pltpu.roll(y, step, 1), y))
            spread.append(jnp.where(upper, y, pltpu.roll(y, LANES - step, 1)))
        out = spread
        step //= 2
    return out


def group_sum(x, capacity):
    lane = lax.broadcasted_iota(jnp.int32, x.shape, 1)
    step = capacity // 2
    while step:
        upper = (lane & step) != 0
        x = x + jnp.where(upper, pltpu.roll(x, step, 1), pltpu.roll(x, LANES - step, 1))
        step //= 2
    return x


def lambda_kernel(
    capacity, part_rows, place_ref, got_ref, pre_ref, slot_ref, w2_ref, emb_ref,
    parts_ref, pre_grad_ref, score_by, mark_by, key_by, disc_by, row_scratch,
):
    sources = got_ref.shape[0]
    halves = got_ref.shape[1] // 4
    me, my_half = place_ref[0], place_ref[1]
    rows = pre_ref.shape[0]
    source = lax.broadcasted_iota(jnp.int32, (sources, LANES), 0)
    lane = lax.broadcasted_iota(jnp.int32, (sources, LANES), 1)
    position = (source * capacity + lane % capacity).astype(jnp.float32)
    slots = float(sources * capacity)
    lane_of_row = lax.broadcasted_iota(jnp.int32, (rows, LANES), 1)
    lambda_column = jnp.zeros((rows, 1), jnp.float32)
    for h in range(halves):
        half_score = got_ref[:, h, :] * 0.5
        mark = got_ref[:, halves + h, :]
        label = got_ref[:, 2 * halves + h, :]
        key = label * slots - position
        for ref, value in ((score_by, half_score), (mark_by, mark), (key_by, key)):
            for c, spread in enumerate(within_groups(value, capacity)):
                ref[c * sources : (c + 1) * sources, :] = spread

        def rank_step(step, sums):
            soft, ideal = sums
            base = pl.multiple_of(step * 8, 8)
            score_rows = score_by[pl.ds(base, 8), :]
            mark_rows = mark_by[pl.ds(base, 8), :]
            key_rows = key_by[pl.ds(base, 8), :]
            for r in range(8):
                same = mark_rows[r : r + 1, :] == mark
                tilt = jnp.tanh(score_rows[r : r + 1, :] - half_score)
                soft = soft + jnp.where(same, tilt + 1.0, 0.0)
                ideal = ideal + jnp.where(same & (key_rows[r : r + 1, :] > key), 1.0, 0.0)
            return soft, ideal

        nothing = jnp.zeros((sources, LANES), jnp.float32)
        soft, ideal = lax.fori_loop(0, capacity * sources // 8, rank_step, (nothing, nothing))
        discount = 1.0 / jnp.log2(2.0 + (0.5 * soft - 0.5))
        gain = jnp.exp2(label) - 1.0
        term = gain / jnp.log2(2.0 + ideal)
        for c, spread in enumerate(within_groups(discount, capacity)):
            disc_by[c * sources : (c + 1) * sources, :] = spread

        for place, value in enumerate((half_score, mark, gain, discount)):
            row_scratch[place * sources : (place + 1) * sources, :] = value
        own_score, own_mark, own_gain, own_disc = (
            row_scratch[pl.ds(place * sources + me, 1), :] for place in range(4)
        )
        ideal_sum = jnp.zeros((1, LANES), jnp.float32)
        for query in range(2):
            asked = query + 1.0
            per_lane = jnp.sum(jnp.where(mark == asked, term, 0.0), axis=0, keepdims=True)
            spread = group_sum(jnp.broadcast_to(per_lane, (8, LANES)), capacity)[:1, :]
            ideal_sum = jnp.where(own_mark == asked, spread, ideal_sum)
        inv_ideal = jnp.where(ideal_sum > 0.0, 1.0 / jnp.where(ideal_sum > 0.0, ideal_sum, 1.0), 0.0)

        total = jnp.zeros((sources, LANES), jnp.float32)
        for c in range(capacity):
            at = slice(c * sources, (c + 1) * sources)
            their_gain = jnp.exp2(jnp.ceil(key_by[at, :] * (1.0 / slots))) - 1.0
            gain_gap = own_gain - their_gain
            gap = 2.0 * (score_by[at, :] - own_score)
            pull = jax.nn.sigmoid(jnp.where(gain_gap > 0.0, gap, -gap))
            pair = -gain_gap * jnp.abs(own_disc - disc_by[at, :]) * pull
            total = total + jnp.where(mark_by[at, :] == own_mark, pair, 0.0)
        lambda_row = jnp.sum(total, axis=0, keepdims=True) * inv_ideal
        here = slot_ref[...] == lane_of_row + h * LANES
        lambda_column = lambda_column + jnp.sum(
            jnp.where(here, lambda_row, 0.0), axis=1, keepdims=True
        )

    pre_act = pre_ref[...]
    gate = jax.nn.sigmoid(pre_act)
    slope = gate * (1.0 + pre_act * (1.0 - gate))
    pre_grad = (lambda_column * w2_ref[...] * slope).astype(jnp.bfloat16)
    pre_grad_ref[...] = pre_grad
    second = jnp.sum(lambda_column * (pre_act * gate), axis=0, keepdims=True)
    columns = pre_act.shape[1] // LANES
    keep_rows = part_rows * columns
    for half in range(2):
        for b in range(parts_ref.shape[1]):
            for k in range(columns):
                parts_ref[half, b, keep_rows + k : keep_rows + k + 1, :] = second[
                    :, k * LANES : (k + 1) * LANES
                ].astype(jnp.bfloat16)
    for b in range(parts_ref.shape[1]):
        product = lax.dot_general(
            emb_ref[:, b * 2 * part_rows : (b + 1) * 2 * part_rows],
            pre_grad,
            (((0,), (0,)), ((), ())),
            preferred_element_type=jnp.float32,
        ).astype(jnp.bfloat16)
        for half in range(2):
            goes_to = (half + my_half) % 2
            for k in range(columns):
                parts_ref[goes_to, b, k * part_rows : (k + 1) * part_rows, :] = product[
                    half * part_rows : (half + 1) * part_rows, k * LANES : (k + 1) * LANES
                ]


def sent_to_all(x, axis):
    count = lax.axis_size(axis)
    return lax.all_to_all(jnp.broadcast_to(x[None], (count, *x.shape)), axis, 0, 0, tiled=True)


def on_device(embeddings, owner_shard, query_local, labels, w_first, w_second):
    docs, lanes, subs = (lax.axis_size(axis) for axis in ("docs", "mp", "sub"))
    rows, width = embeddings.shape
    units = w_first.shape[1]
    capacity = 2 * rows // docs
    halves = docs * capacity // LANES
    w2_row = w_second.reshape(1, units)
    sent, pre_act, slot = pl.pallas_call(
        functools.partial(score_kernel, capacity),
        out_shape=(
            whole((4 * halves, LANES), jnp.float32),
            whole((rows, units), jnp.float32),
            whole((rows, 1), jnp.int32),
        ),
        in_specs=vmem_specs(6),
        out_specs=tuple(vmem_specs(3)),
        name="score",
    )(
        embeddings, w_first, w2_row,
        owner_shard.reshape(1, rows), query_local.reshape(1, rows), labels.reshape(1, rows),
    )
    got = sent_to_all(sent, "docs")

    part_rows = width // (lanes * subs)
    columns = units // LANES
    place = jnp.stack([lax.axis_index("docs"), lax.axis_index("sub")]).astype(jnp.int32)
    parts, pre_grad = pl.pallas_call(
        functools.partial(lambda_kernel, capacity, part_rows),
        out_shape=(
            whole((subs, lanes, (part_rows + 1) * columns, LANES), jnp.bfloat16),
            whole((rows, units), jnp.bfloat16),
        ),
        in_specs=[pl.BlockSpec(memory_space=pltpu.SMEM)] + vmem_specs(5),
        out_specs=tuple(vmem_specs(2)),
        scratch_shapes=[pltpu.VMEM((docs * capacity, LANES), jnp.float32)] * 4
        + [pltpu.VMEM((4 * docs, LANES), jnp.float32)],
        name="lambdas",
    )(place, got, pre_act, slot, w2_row, embeddings)

    other = lax.ppermute(parts[1], "sub", [(0, 1), (1, 0)])
    emb_grad = lax.dot_general(
        pre_grad, w_first, (((1,), (1,)), ((), ())), preferred_element_type=jnp.float32
    ).astype(jnp.bfloat16)
    chip_sum = (parts[0].astype(jnp.float32) + other.astype(jnp.float32)).astype(jnp.bfloat16)
    arrived = lax.all_to_all(chip_sum, "mp", 0, 0, tiled=True)
    line_sum = arrived.astype(jnp.float32).sum(axis=0).astype(jnp.bfloat16)
    first_rows = part_rows * columns
    tiles = line_sum[:first_rows].reshape(docs, first_rows // docs, LANES)
    second = jnp.broadcast_to(line_sum[first_rows:][None], (docs, columns, LANES))
    arrived = lax.all_to_all(jnp.concatenate([tiles, second], axis=1), "docs", 0, 0, tiled=True)
    shard_sum = arrived.astype(jnp.float32).sum(axis=0)
    w_second_grad = shard_sum[first_rows // docs :].reshape(units)
    spread = sent_to_all(shard_sum[: first_rows // docs].astype(jnp.bfloat16), "docs")
    w_first_grad = (
        spread.reshape(columns, part_rows, LANES).transpose(1, 0, 2).reshape(part_rows, units)
    ).astype(jnp.float32)
    return (emb_grad, w_first_grad, w_second_grad)


def solution(mesh):
    split = ("groups", "docs", "mp", "sub")
    return jax.shard_map(
        on_device,
        mesh=mesh,
        in_specs=(P(split, None), P(split, None), P(split), P(split), P(), P()),
        out_specs=(P(split, None), P(("groups", "mp", "sub"), None), P("groups")),
        check_vma=False,
    )
```

```python
import functools

import jax
import jax.numpy as jnp
from jax import lax
from jax.experimental import pallas as pl
from jax.experimental.pallas import tpu as pltpu
from jax.sharding import PartitionSpec as P

LANES = 128
FAR = (3, 4, 5)
NEAR = (0, 1, 2, 6, 7)


def whole(*shape_and_type):
    return jax.ShapeDtypeStruct(*shape_and_type)


def vmem_specs(count):
    return [pl.BlockSpec(memory_space=pltpu.VMEM)] * count


def score_kernel(capacity, emb_ref, w1_ref, w2_ref, owner_ref, query_ref, label_ref, sent_ref, pre_ref, slot_ref):
    rows = emb_ref.shape[0]
    halves = sent_ref.shape[1] // 4
    along = lax.broadcasted_iota(jnp.int32, (rows, rows), 1)
    down = lax.broadcasted_iota(jnp.int32, (rows, rows), 0)

    def column(row):
        return jnp.sum(jnp.where(along == down, row, 0), axis=1, keepdims=True)

    owner = owner_ref[...]
    owner_column = column(owner)
    earlier = jnp.where((owner_column == owner) & (along < down), 1, 0)
    slot = owner_column * capacity + jnp.sum(earlier, axis=1, keepdims=True)
    slot_ref[...] = slot
    mark = column(query_ref[...] + 1).astype(jnp.float32)
    label = column(label_ref[...]).astype(jnp.float32)

    pre_act = jnp.dot(emb_ref[...], w1_ref[...], preferred_element_type=jnp.float32)
    pre_ref[...] = pre_act
    hidden = pre_act * jax.nn.sigmoid(pre_act)
    score = jnp.sum(hidden * w2_ref[...], axis=1, keepdims=True)

    lane = lax.broadcasted_iota(jnp.int32, (rows, LANES), 1)
    sent_ref[...] = jnp.zeros_like(sent_ref)
    for h in range(halves):
        here = slot == lane + h * LANES
        for place, value in enumerate((score, mark, label)):
            row = jnp.sum(jnp.where(here, value, 0.0), axis=0, keepdims=True)
            for target in range(sent_ref.shape[0]):
                sent_ref[target, place * halves + h : place * halves + h + 1, :] = row


def within_groups(x, capacity):
    lane = lax.broadcasted_iota(jnp.int32, x.shape, 1)
    out = [x]
    step = capacity // 2
    while step:
        upper = (lane & step) != 0
        spread = []
        for y in out:
            spread.append(jnp.where(upper, pltpu.roll(y, step, 1), y))
            spread.append(jnp.where(upper, y, pltpu.roll(y, LANES - step, 1)))
        out = spread
        step //= 2
    return out


def group_sum(x, capacity):
    lane = lax.broadcasted_iota(jnp.int32, x.shape, 1)
    step = capacity // 2
    while step:
        upper = (lane & step) != 0
        x = x + jnp.where(upper, pltpu.roll(x, step, 1), pltpu.roll(x, LANES - step, 1))
        step //= 2
    return x


def lambda_kernel(
    capacity, part_rows, place_ref, got_ref, pre_ref, slot_ref, w2_ref, emb_ref,
    keep_far_ref, keep_near_ref, send_far_ref, send_near_ref, pre_grad_ref, score_by, mark_by, key_by, disc_by, row_scratch,
):
    sources = got_ref.shape[0]
    halves = got_ref.shape[1] // 4
    me, my_half, my_lane = place_ref[0], place_ref[1], place_ref[2]
    rows = pre_ref.shape[0]
    source = lax.broadcasted_iota(jnp.int32, (sources, LANES), 0)
    lane = lax.broadcasted_iota(jnp.int32, (sources, LANES), 1)
    position = (source * capacity + lane % capacity).astype(jnp.float32)
    slots = float(sources * capacity)
    lane_of_row = lax.broadcasted_iota(jnp.int32, (rows, LANES), 1)
    lambda_column = jnp.zeros((rows, 1), jnp.float32)
    for h in range(halves):
        half_score = got_ref[:, h, :] * 0.5
        mark = got_ref[:, halves + h, :]
        label = got_ref[:, 2 * halves + h, :]
        key = label * slots - position
        for ref, value in ((score_by, half_score), (mark_by, mark), (key_by, key)):
            for c, spread in enumerate(within_groups(value, capacity)):
                ref[c * sources : (c + 1) * sources, :] = spread

        def rank_step(step, sums):
            soft, ideal = sums
            base = pl.multiple_of(step * 8, 8)
            score_rows = score_by[pl.ds(base, 8), :]
            mark_rows = mark_by[pl.ds(base, 8), :]
            key_rows = key_by[pl.ds(base, 8), :]
            for r in range(8):
                same = mark_rows[r : r + 1, :] == mark
                tilt = jnp.tanh(score_rows[r : r + 1, :] - half_score)
                soft = soft + jnp.where(same, tilt + 1.0, 0.0)
                ideal = ideal + jnp.where(same & (key_rows[r : r + 1, :] > key), 1.0, 0.0)
            return soft, ideal

        nothing = jnp.zeros((sources, LANES), jnp.float32)
        soft, ideal = lax.fori_loop(0, capacity * sources // 8, rank_step, (nothing, nothing))
        discount = 1.0 / jnp.log2(2.0 + (0.5 * soft - 0.5))
        gain = jnp.exp2(label) - 1.0
        term = gain / jnp.log2(2.0 + ideal)
        for c, spread in enumerate(within_groups(discount, capacity)):
            disc_by[c * sources : (c + 1) * sources, :] = spread

        for place, value in enumerate((half_score, mark, gain, discount)):
            row_scratch[place * sources : (place + 1) * sources, :] = value
        own_score, own_mark, own_gain, own_disc = (
            row_scratch[pl.ds(place * sources + me, 1), :] for place in range(4)
        )
        ideal_sum = jnp.zeros((1, LANES), jnp.float32)
        for query in range(2):
            asked = query + 1.0
            per_lane = jnp.sum(jnp.where(mark == asked, term, 0.0), axis=0, keepdims=True)
            spread = group_sum(jnp.broadcast_to(per_lane, (8, LANES)), capacity)[:1, :]
            ideal_sum = jnp.where(own_mark == asked, spread, ideal_sum)
        inv_ideal = jnp.where(ideal_sum > 0.0, 1.0 / jnp.where(ideal_sum > 0.0, ideal_sum, 1.0), 0.0)

        total = jnp.zeros((sources, LANES), jnp.float32)
        for c in range(capacity):
            at = slice(c * sources, (c + 1) * sources)
            their_gain = jnp.exp2(jnp.ceil(key_by[at, :] * (1.0 / slots))) - 1.0
            gain_gap = own_gain - their_gain
            gap = 2.0 * (score_by[at, :] - own_score)
            pull = jax.nn.sigmoid(jnp.where(gain_gap > 0.0, gap, -gap))
            pair = -gain_gap * jnp.abs(own_disc - disc_by[at, :]) * pull
            total = total + jnp.where(mark_by[at, :] == own_mark, pair, 0.0)
        lambda_row = jnp.sum(total, axis=0, keepdims=True) * inv_ideal
        here = slot_ref[...] == lane_of_row + h * LANES
        lambda_column = lambda_column + jnp.sum(
            jnp.where(here, lambda_row, 0.0), axis=1, keepdims=True
        )

    pre_act = pre_ref[...]
    gate = jax.nn.sigmoid(pre_act)
    slope = gate * (1.0 + pre_act * (1.0 - gate))
    pre_grad = (lambda_column * w2_ref[...] * slope).astype(jnp.bfloat16)
    pre_grad_ref[...] = pre_grad
    second = jnp.sum(lambda_column * (pre_act * gate), axis=0, keepdims=True)
    columns = pre_act.shape[1] // LANES
    keep_rows = part_rows * columns
    lanes = keep_far_ref.shape[0] + keep_near_ref.shape[0]
    places = [(keep_far_ref, send_far_ref, i) for i in range(len(FAR))]
    places += [(keep_near_ref, send_near_ref, i) for i in range(len(NEAR))]
    second_rows = [
        second[:, k * LANES : (k + 1) * LANES].astype(jnp.bfloat16) for k in range(columns)
    ]
    for distance, (keep_ref, send_ref, i) in zip(FAR + NEAR, places, strict=True):
        block = lax.rem(my_lane + distance, lanes)
        product = lax.dot_general(
            emb_ref[:, pl.ds(pl.multiple_of(block * 2 * part_rows, LANES), 2 * part_rows)],
            pre_grad,
            (((0,), (0,)), ((), ())),
            preferred_element_type=jnp.float32,
        )
        top, bottom = product[:part_rows], product[part_rows:]
        keep = jnp.where(my_half == 0, top, bottom).astype(jnp.bfloat16)
        send = jnp.where(my_half == 0, bottom, top).astype(jnp.bfloat16)
        for ref, value in ((keep_ref, keep), (send_ref, send)):
            for k in range(columns):
                ref[i, k * part_rows : (k + 1) * part_rows, :] = value[:, k * LANES : (k + 1) * LANES]
                ref[i, keep_rows + k : keep_rows + k + 1, :] = second_rows[k]


def sent_to_all(x, axis):
    count = lax.axis_size(axis)
    return lax.all_to_all(jnp.broadcast_to(x[None], (count, *x.shape)), axis, 0, 0, tiled=True)


def on_device(embeddings, owner_shard, query_local, labels, w_first, w_second):
    docs, lanes, subs = (lax.axis_size(axis) for axis in ("docs", "mp", "sub"))
    rows, width = embeddings.shape
    units = w_first.shape[1]
    capacity = 2 * rows // docs
    halves = docs * capacity // LANES
    w2_row = w_second.reshape(1, units)
    sent, pre_act, slot = pl.pallas_call(
        functools.partial(score_kernel, capacity),
        out_shape=(
            whole((docs, 4 * halves, LANES), jnp.float32),
            whole((rows, units), jnp.float32),
            whole((rows, 1), jnp.int32),
        ),
        in_specs=vmem_specs(6),
        out_specs=tuple(vmem_specs(3)),
        name="score",
    )(
        embeddings, w_first, w2_row,
        owner_shard.reshape(1, rows), query_local.reshape(1, rows), labels.reshape(1, rows),
    )
    got = lax.all_to_all(sent, "docs", 0, 0, tiled=True)

    part_rows = width // (lanes * subs)
    columns = units // LANES
    tall = (part_rows + 1) * columns
    far, near = (len(FAR), tall, LANES), (len(NEAR), tall, LANES)
    my_half = lax.axis_index("sub")
    place = jnp.stack([lax.axis_index("docs"), my_half, lax.axis_index("mp")]).astype(jnp.int32)
    keep_far, keep_near, send_far, send_near, pre_grad = pl.pallas_call(
        functools.partial(lambda_kernel, capacity, part_rows),
        out_shape=tuple(whole(shape, jnp.bfloat16) for shape in (far, near, far, near, (rows, units))),
        in_specs=[pl.BlockSpec(memory_space=pltpu.SMEM)] + vmem_specs(5),
        out_specs=tuple(vmem_specs(5)),
        scratch_shapes=[pltpu.VMEM((docs * capacity, LANES), jnp.float32)] * 4
        + [pltpu.VMEM((4 * docs, LANES), jnp.float32)],
        name="lambdas",
    )(place, got, pre_act, slot, w2_row, embeddings)

    swap = [(0, 1), (1, 0)]
    far_in = lax.ppermute(send_far, "sub", swap)
    near_in = lax.ppermute(send_near, "sub", swap)

    emb_grad = lax.dot_general(
        pre_grad, w_first, (((1,), (1,)), ((), ())), preferred_element_type=jnp.float32
    ).astype(jnp.bfloat16)

    def moved(x, by):
        return lax.ppermute(x, "mp", [(i, (i + by) % lanes) for i in range(lanes)])

    def added(*terms):
        return sum(term.astype(jnp.float32) for term in terms).astype(jnp.bfloat16)

    ahead, across, behind = (added(keep_far[i], far_in[i]) for i in range(3))
    both_ways = [
        (i * subs + s, (i + (2 if s == 0 else -2)) % lanes * subs + s)
        for i in range(lanes)
        for s in range(subs)
    ]
    across = lax.ppermute(across, ("mp", "sub"), both_ways)
    ahead, behind = moved(ahead, 1), moved(behind, -1)
    zero, one, two, six, seven = (
        keep_near[i].astype(jnp.float32) + near_in[i].astype(jnp.float32) for i in range(5)
    )
    none = jnp.zeros_like(across)
    two = moved(added(two, ahead, jnp.where(my_half == 0, across, none)), 2)
    six = moved(added(six, behind, jnp.where(my_half == 0, none, across)), -2)
    one, seven = moved(one.astype(jnp.bfloat16), 1), moved(seven.astype(jnp.bfloat16), -1)
    line_sum = added(zero, two, six, one, seven)
    first_rows = part_rows * columns
    tiles = line_sum[:first_rows].reshape(docs, first_rows // docs, LANES)
    second = jnp.broadcast_to(line_sum[first_rows:][None], (docs, columns, LANES))
    arrived = lax.all_to_all(jnp.concatenate([tiles, second], axis=1), "docs", 0, 0, tiled=True)
    shard_sum = arrived.astype(jnp.float32).sum(axis=0)
    w_second_grad = shard_sum[first_rows // docs :].reshape(units)
    spread = sent_to_all(shard_sum[: first_rows // docs].astype(jnp.bfloat16), "docs")
    w_first_grad = (
        spread.reshape(columns, part_rows, LANES).transpose(1, 0, 2).reshape(part_rows, units)
    ).astype(jnp.float32)
    return (emb_grad, w_first_grad, w_second_grad)


def solution(mesh):
    split = ("groups", "docs", "mp", "sub")
    return jax.shard_map(
        on_device,
        mesh=mesh,
        in_specs=(P(split, None), P(split, None), P(split), P(split), P(), P()),
        out_specs=(P(split, None), P(("groups", "mp", "sub"), None), P("groups")),
        check_vma=False,
    )
```

```python
import functools

import jax
import jax.numpy as jnp
from jax import lax
from jax.experimental import pallas as pl
from jax.experimental.pallas import tpu as pltpu
from jax.sharding import PartitionSpec as P

LANES = 128


def whole(*shape_and_type):
    return jax.ShapeDtypeStruct(*shape_and_type)


def vmem_specs(count):
    return [pl.BlockSpec(memory_space=pltpu.VMEM)] * count


def score_kernel(capacity, emb_ref, w1_ref, w2_ref, owner_ref, query_ref, label_ref, sent_ref, slot_ref):
    rows = emb_ref.shape[0]
    halves = sent_ref.shape[1] // 4
    along = lax.broadcasted_iota(jnp.int32, (rows, rows), 1)
    down = lax.broadcasted_iota(jnp.int32, (rows, rows), 0)

    def column(row):
        return jnp.sum(jnp.where(along == down, row, 0), axis=1, keepdims=True)

    owner = owner_ref[...]
    owner_column = column(owner)
    earlier = jnp.where((owner_column == owner) & (along < down), 1, 0)
    slot = owner_column * capacity + jnp.sum(earlier, axis=1, keepdims=True)
    slot_ref[...] = slot
    mark = column(query_ref[...] + 1).astype(jnp.float32)
    label = column(label_ref[...]).astype(jnp.float32)

    pre_act = jnp.dot(emb_ref[...], w1_ref[...], preferred_element_type=jnp.float32)
    hidden = pre_act * jax.nn.sigmoid(pre_act)
    score = jnp.sum(hidden * w2_ref[...], axis=1, keepdims=True)

    lane = lax.broadcasted_iota(jnp.int32, (rows, LANES), 1)
    sent_ref[...] = jnp.zeros_like(sent_ref)
    for h in range(halves):
        here = slot == lane + h * LANES
        for place, value in enumerate((score, mark, label)):
            row = jnp.sum(jnp.where(here, value, 0.0), axis=0, keepdims=True)
            for target in range(sent_ref.shape[0]):
                sent_ref[target, place * halves + h : place * halves + h + 1, :] = row


def within_groups(x, capacity):
    lane = lax.broadcasted_iota(jnp.int32, x.shape, 1)
    out = [x]
    step = capacity // 2
    while step:
        upper = (lane & step) != 0
        spread = []
        for y in out:
            spread.append(jnp.where(upper, pltpu.roll(y, step, 1), y))
            spread.append(jnp.where(upper, y, pltpu.roll(y, LANES - step, 1)))
        out = spread
        step //= 2
    return out


def group_sum(x, capacity):
    lane = lax.broadcasted_iota(jnp.int32, x.shape, 1)
    step = capacity // 2
    while step:
        upper = (lane & step) != 0
        x = x + jnp.where(upper, pltpu.roll(x, step, 1), pltpu.roll(x, LANES - step, 1))
        step //= 2
    return x


def lambda_kernel(
    capacity, place_ref, got_ref, slot_ref, spread_ref, column_ref,
    score_by, mark_by, key_by, disc_by, row_scratch,
):
    sources = got_ref.shape[0]
    halves = got_ref.shape[1] // 4
    me = place_ref[0]
    rows = slot_ref.shape[0]
    source = lax.broadcasted_iota(jnp.int32, (sources, LANES), 0)
    lane = lax.broadcasted_iota(jnp.int32, (sources, LANES), 1)
    position = (source * capacity + lane % capacity).astype(jnp.float32)
    slots = float(sources * capacity)
    lane_of_row = lax.broadcasted_iota(jnp.int32, (rows, LANES), 1)
    lambda_column = jnp.zeros((rows, 1), jnp.float32)
    for h in range(halves):
        half_score = got_ref[:, h, :] * 0.5
        mark = got_ref[:, halves + h, :]
        label = got_ref[:, 2 * halves + h, :]
        key = label * slots - position
        for ref, value in ((score_by, half_score), (mark_by, mark), (key_by, key)):
            for c, spread in enumerate(within_groups(value, capacity)):
                ref[c * sources : (c + 1) * sources, :] = spread

        def rank_step(step, sums):
            soft, ideal = sums
            base = pl.multiple_of(step * 8, 8)
            score_rows = score_by[pl.ds(base, 8), :]
            mark_rows = mark_by[pl.ds(base, 8), :]
            key_rows = key_by[pl.ds(base, 8), :]
            for r in range(8):
                same = mark_rows[r : r + 1, :] == mark
                tilt = jnp.tanh(score_rows[r : r + 1, :] - half_score)
                soft = soft + jnp.where(same, tilt + 1.0, 0.0)
                ideal = ideal + jnp.where(same & (key_rows[r : r + 1, :] > key), 1.0, 0.0)
            return soft, ideal

        nothing = jnp.zeros((sources, LANES), jnp.float32)
        soft, ideal = lax.fori_loop(0, capacity * sources // 8, rank_step, (nothing, nothing))
        discount = 1.0 / jnp.log2(2.0 + (0.5 * soft - 0.5))
        gain = jnp.exp2(label) - 1.0
        term = gain / jnp.log2(2.0 + ideal)
        for c, spread in enumerate(within_groups(discount, capacity)):
            disc_by[c * sources : (c + 1) * sources, :] = spread

        for place, value in enumerate((half_score, mark, gain, discount)):
            row_scratch[place * sources : (place + 1) * sources, :] = value
        own_score, own_mark, own_gain, own_disc = (
            row_scratch[pl.ds(place * sources + me, 1), :] for place in range(4)
        )
        ideal_sum = jnp.zeros((1, LANES), jnp.float32)
        for query in range(2):
            asked = query + 1.0
            per_lane = jnp.sum(jnp.where(mark == asked, term, 0.0), axis=0, keepdims=True)
            spread = group_sum(jnp.broadcast_to(per_lane, (8, LANES)), capacity)[:1, :]
            ideal_sum = jnp.where(own_mark == asked, spread, ideal_sum)
        inv_ideal = jnp.where(ideal_sum > 0.0, 1.0 / jnp.where(ideal_sum > 0.0, ideal_sum, 1.0), 0.0)

        total = jnp.zeros((sources, LANES), jnp.float32)
        for c in range(capacity):
            at = slice(c * sources, (c + 1) * sources)
            their_gain = jnp.exp2(jnp.ceil(key_by[at, :] * (1.0 / slots))) - 1.0
            gain_gap = own_gain - their_gain
            gap = 2.0 * (score_by[at, :] - own_score)
            pull = jax.nn.sigmoid(jnp.where(gain_gap > 0.0, gap, -gap))
            pair = -gain_gap * jnp.abs(own_disc - disc_by[at, :]) * pull
            total = total + jnp.where(mark_by[at, :] == own_mark, pair, 0.0)
        lambda_row = jnp.sum(total, axis=0, keepdims=True) * inv_ideal
        here = slot_ref[...] == lane_of_row + h * LANES
        lambda_column = lambda_column + jnp.sum(
            jnp.where(here, lambda_row, 0.0), axis=1, keepdims=True
        )

    column_ref[...] = lambda_column
    along = lax.broadcasted_iota(jnp.int32, (rows, rows), 1)
    down = lax.broadcasted_iota(jnp.int32, (rows, rows), 0)
    row = jnp.sum(jnp.where(along == down, lambda_column, 0.0), axis=0, keepdims=True)
    spread_ref[...] = jnp.broadcast_to(row[None], spread_ref.shape)


def slope_kernel(count, place_ref, w1_ref, w2_ref, *refs):
    emb_refs, (slope_ref, hidden_ref, part_ref) = refs[:count], refs[count:]
    wide = part_ref.shape[2]
    mine = pl.ds(pl.multiple_of(place_ref[1] * wide, LANES), wide)
    for i, emb_ref in enumerate(emb_refs):
        pre_act = jnp.dot(emb_ref[...], w1_ref[...], preferred_element_type=jnp.float32)
        gate = jax.nn.sigmoid(pre_act)
        hidden_ref[i] = (pre_act * gate).astype(jnp.bfloat16)
        slope = gate * (1.0 + pre_act * (1.0 - gate))
        slope_ref[i] = (w2_ref[...] * slope).astype(jnp.bfloat16)
        part_ref[i] = emb_ref[:, mine]


def slopes(place, w_first, w2_row, blocks, wide):
    rows, units = blocks[0].shape[0], w_first.shape[1]
    count = len(blocks)
    return pl.pallas_call(
        functools.partial(slope_kernel, count),
        out_shape=(
            whole((count, rows, units), jnp.bfloat16),
            whole((count, rows, units), jnp.bfloat16),
            whole((count, rows, wide), jnp.bfloat16),
        ),
        in_specs=[pl.BlockSpec(memory_space=pltpu.SMEM)] + vmem_specs(2 + count),
        out_specs=tuple(vmem_specs(3)),
        name="slopes",
    )(place, w_first, w2_row, *blocks)


def product_kernel(groups, place_ref, lambda_ref, *refs):
    inputs, (keep_ref, send_ref) = refs[: 3 * len(groups)], refs[3 * len(groups) :]
    my_lane, my_half = place_ref[1], place_ref[2]
    lanes, rows = lambda_ref.shape[0], lambda_ref.shape[2]
    along = lax.broadcasted_iota(jnp.int32, (rows, rows), 1)
    down = lax.broadcasted_iota(jnp.int32, (rows, rows), 0)
    total, second = None, None
    for g, offsets in enumerate(groups):
        slope_ref, hidden_ref, part_ref = inputs[3 * g : 3 * g + 3]
        for i, offset in enumerate(offsets):
            block = lambda_ref[lax.rem(my_lane + offset + lanes, lanes)]
            column = jnp.sum(jnp.where(along == down, block[:1], 0.0), axis=1, keepdims=True)
            part = (part_ref[i].astype(jnp.float32) * column).astype(jnp.bfloat16)
            product = lax.dot_general(
                part, slope_ref[i], (((0,), (0,)), ((), ())), preferred_element_type=jnp.float32
            )
            high = block.astype(jnp.bfloat16)
            low = (block - high.astype(jnp.float32)).astype(jnp.bfloat16)
            hidden = hidden_ref[i]
            summed = jnp.dot(high, hidden, preferred_element_type=jnp.float32) + jnp.dot(
                low, hidden, preferred_element_type=jnp.float32
            )
            total = product if total is None else total + product
            second = summed if second is None else second + summed
    half_rows = total.shape[0] // 2
    columns = total.shape[1] // LANES
    top, bottom = total[:half_rows], total[half_rows:]
    keep = jnp.where(my_half == 0, top, bottom).astype(jnp.bfloat16)
    send = jnp.where(my_half == 0, bottom, top).astype(jnp.bfloat16)
    for ref, value in ((keep_ref, keep), (send_ref, send)):
        for k in range(columns):
            at = slice(k * LANES, (k + 1) * LANES)
            ref[k * half_rows : (k + 1) * half_rows, :] = value[:, at]
            row = half_rows * columns + k
            ref[row : row + 1, :] = second[:1, at].astype(jnp.bfloat16)


def sent_to_all(x, axis):
    count = lax.axis_size(axis)
    return lax.all_to_all(jnp.broadcast_to(x[None], (count, *x.shape)), axis, 0, 0, tiled=True)


def plane_blocks(block):
    lanes, subs = lax.axis_size("mp"), lax.axis_size("sub")

    def moved(x, by):
        return lax.ppermute(x, "mp", [(i, (i + by) % lanes) for i in range(lanes)])

    two_back, two_on = moved(block, 2), moved(block, -2)
    one_back, one_on = moved(block, 1), moved(block, -1)
    three_back, three_on = moved(two_back, 1), moved(two_on, -1)
    both_ways = [
        (i * subs + s, (i + (2 if s == 0 else -2)) % lanes * subs + s)
        for i in range(lanes)
        for s in range(subs)
    ]
    passed = jnp.where(lax.axis_index("sub") == 0, two_back, two_on)
    across = lax.ppermute(passed, ("mp", "sub"), both_ways)
    near = {-2: two_back, 2: two_on, -1: one_back, 1: one_on}
    far = {-3: three_back, 3: three_on, 4: across}
    return near, far


def on_device(embeddings, owner_shard, query_local, labels, w_first, w_second):
    docs, lanes, subs = (lax.axis_size(axis) for axis in ("docs", "mp", "sub"))
    rows, width = embeddings.shape
    units = w_first.shape[1]
    capacity = 2 * rows // docs
    halves = docs * capacity // LANES
    w2_row = w_second.reshape(1, units)
    place = jnp.stack([lax.axis_index(axis) for axis in ("docs", "mp", "sub")]).astype(jnp.int32)
    near, far = plane_blocks(embeddings)
    sent, slot = pl.pallas_call(
        functools.partial(score_kernel, capacity),
        out_shape=(
            whole((docs, 4 * halves, LANES), jnp.float32),
            whole((rows, 1), jnp.int32),
        ),
        in_specs=vmem_specs(6),
        out_specs=tuple(vmem_specs(2)),
        name="score",
    )(
        embeddings, w_first, w2_row,
        owner_shard.reshape(1, rows), query_local.reshape(1, rows), labels.reshape(1, rows),
    )
    got = lax.all_to_all(sent, "docs", 0, 0, tiled=True)
    spread, lambda_column = pl.pallas_call(
        functools.partial(lambda_kernel, capacity),
        out_shape=(whole((lanes, 8, rows), jnp.float32), whole((rows, 1), jnp.float32)),
        in_specs=[pl.BlockSpec(memory_space=pltpu.SMEM)] + vmem_specs(2),
        out_specs=tuple(vmem_specs(2)),
        scratch_shapes=[pltpu.VMEM((docs * capacity, LANES), jnp.float32)] * 4
        + [pltpu.VMEM((4 * docs, LANES), jnp.float32)],
        name="lambdas",
    )(place, got, slot)
    all_lambdas = lax.all_to_all(spread, "mp", 0, 0, tiled=True)

    part_rows = width // (lanes * subs)
    wide = subs * part_rows
    columns = units // LANES
    own = slopes(place, w_first, w2_row, [embeddings], wide)
    beside = slopes(place, w_first, w2_row, list(near.values()), wide)
    beyond = slopes(place, w_first, w2_row, list(far.values()), wide)
    own_grad = lax.dot_general(
        own[0][0], w_first, (((1,), (1,)), ((), ())), preferred_element_type=jnp.float32
    )
    emb_grad = (lambda_column * own_grad).astype(jnp.bfloat16)
    tall = ((part_rows + 1) * columns, LANES)
    keep, send = pl.pallas_call(
        functools.partial(product_kernel, ((0,), tuple(near), tuple(far))),
        out_shape=(whole(tall, jnp.bfloat16), whole(tall, jnp.bfloat16)),
        in_specs=[pl.BlockSpec(memory_space=pltpu.SMEM)] + vmem_specs(10),
        out_specs=tuple(vmem_specs(2)),
        name="product",
    )(place, all_lambdas, *own, *beside, *beyond)
    other = lax.ppermute(send, "sub", [(0, 1), (1, 0)])
    line_sum = (keep.astype(jnp.float32) + other.astype(jnp.float32)).astype(jnp.bfloat16)
    first_rows = part_rows * columns
    tiles = line_sum[:first_rows].reshape(docs, first_rows // docs, LANES)
    second = jnp.broadcast_to(line_sum[first_rows:][None], (docs, columns, LANES))
    arrived = lax.all_to_all(jnp.concatenate([tiles, second], axis=1), "docs", 0, 0, tiled=True)
    shard_sum = arrived.astype(jnp.float32).sum(axis=0)
    w_second_grad = shard_sum[first_rows // docs :].reshape(units)
    spread = sent_to_all(shard_sum[: first_rows // docs].astype(jnp.bfloat16), "docs")
    w_first_grad = (
        spread.reshape(columns, part_rows, LANES).transpose(1, 0, 2).reshape(part_rows, units)
    ).astype(jnp.float32)
    return (emb_grad, w_first_grad, w_second_grad)


def solution(mesh):
    split = ("groups", "docs", "mp", "sub")
    return jax.shard_map(
        on_device,
        mesh=mesh,
        in_specs=(P(split, None), P(split, None), P(split), P(split), P(), P()),
        out_specs=(P(split, None), P(("groups", "mp", "sub"), None), P("groups")),
        check_vma=False,
    )
```

```python
import functools

import jax
import jax.numpy as jnp
from jax import lax
from jax.experimental import pallas as pl
from jax.experimental.pallas import tpu as pltpu
from jax.sharding import PartitionSpec as P


LANES = 128


def whole(*shape_and_type):
    return jax.ShapeDtypeStruct(*shape_and_type)


def vmem_specs(count):
    return [pl.BlockSpec(memory_space=pltpu.VMEM)] * count


def score_kernel(capacity, emb_ref, w1_ref, w2_ref, owner_ref, query_ref, label_ref, sent_ref, slot_ref):
    rows = emb_ref.shape[0]
    halves = sent_ref.shape[1] // 4
    along = lax.broadcasted_iota(jnp.int32, (rows, rows), 1)
    down = lax.broadcasted_iota(jnp.int32, (rows, rows), 0)

    def column(row):
        return jnp.sum(jnp.where(along == down, row, 0), axis=1, keepdims=True)

    owner = owner_ref[...]
    owner_column = column(owner)
    earlier = jnp.where((owner_column == owner) & (along < down), 1, 0)
    slot = owner_column * capacity + jnp.sum(earlier, axis=1, keepdims=True)
    slot_ref[...] = slot
    mark = column(query_ref[...] + 1).astype(jnp.float32)
    label = column(label_ref[...]).astype(jnp.float32)

    pre_act = jnp.dot(emb_ref[...], w1_ref[...], preferred_element_type=jnp.float32)
    hidden = pre_act * jax.nn.sigmoid(pre_act)
    score = jnp.sum(hidden * w2_ref[...], axis=1, keepdims=True)

    lane = lax.broadcasted_iota(jnp.int32, (rows, LANES), 1)
    sent_ref[...] = jnp.zeros_like(sent_ref)
    for h in range(halves):
        here = slot == lane + h * LANES
        for place, value in enumerate((score, mark, label)):
            row = jnp.sum(jnp.where(here, value, 0.0), axis=0, keepdims=True)
            for target in range(sent_ref.shape[0]):
                sent_ref[target, place * halves + h : place * halves + h + 1, :] = row


def within_groups(x, capacity):
    lane = lax.broadcasted_iota(jnp.int32, x.shape, 1)
    out = [x]
    step = capacity // 2
    while step:
        upper = (lane & step) != 0
        spread = []
        for y in out:
            spread.append(jnp.where(upper, pltpu.roll(y, step, 1), y))
            spread.append(jnp.where(upper, y, pltpu.roll(y, LANES - step, 1)))
        out = spread
        step //= 2
    return out


def group_sum(x, capacity):
    lane = lax.broadcasted_iota(jnp.int32, x.shape, 1)
    step = capacity // 2
    while step:
        upper = (lane & step) != 0
        x = x + jnp.where(upper, pltpu.roll(x, step, 1), pltpu.roll(x, LANES - step, 1))
        step //= 2
    return x


def lambda_kernel(
    capacity, place_ref, got_ref, slot_ref, spread_ref, column_ref,
    score_by, mark_by, key_by, disc_by, row_scratch,
):
    sources = got_ref.shape[0]
    halves = got_ref.shape[1] // 4
    me = place_ref[0]
    rows = slot_ref.shape[0]
    source = lax.broadcasted_iota(jnp.int32, (sources, LANES), 0)
    lane = lax.broadcasted_iota(jnp.int32, (sources, LANES), 1)
    position = (source * capacity + lane % capacity).astype(jnp.float32)
    slots = float(sources * capacity)
    lane_of_row = lax.broadcasted_iota(jnp.int32, (rows, LANES), 1)
    lambda_column = jnp.zeros((rows, 1), jnp.float32)
    for h in range(halves):
        half_score = got_ref[:, h, :] * 0.5
        mark = got_ref[:, halves + h, :]
        label = got_ref[:, 2 * halves + h, :]
        key = label * slots - position
        for ref, value in ((score_by, half_score), (mark_by, mark), (key_by, key)):
            for c, spread in enumerate(within_groups(value, capacity)):
                ref[c * sources : (c + 1) * sources, :] = spread

        def rank_step(step, sums):
            soft, ideal = sums
            base = pl.multiple_of(step * 8, 8)
            score_rows = score_by[pl.ds(base, 8), :]
            mark_rows = mark_by[pl.ds(base, 8), :]
            key_rows = key_by[pl.ds(base, 8), :]
            for r in range(8):
                same = mark_rows[r : r + 1, :] == mark
                tilt = jnp.tanh(score_rows[r : r + 1, :] - half_score)
                soft = soft + jnp.where(same, tilt + 1.0, 0.0)
                ideal = ideal + jnp.where(same & (key_rows[r : r + 1, :] > key), 1.0, 0.0)
            return soft, ideal

        nothing = jnp.zeros((sources, LANES), jnp.float32)
        soft, ideal = lax.fori_loop(0, capacity * sources // 8, rank_step, (nothing, nothing))
        discount = 1.0 / jnp.log2(2.0 + (0.5 * soft - 0.5))
        gain = jnp.exp2(label) - 1.0
        term = gain / jnp.log2(2.0 + ideal)
        for c, spread in enumerate(within_groups(discount, capacity)):
            disc_by[c * sources : (c + 1) * sources, :] = spread

        for place, value in enumerate((half_score, mark, gain, discount)):
            row_scratch[place * sources : (place + 1) * sources, :] = value
        own_score, own_mark, own_gain, own_disc = (
            row_scratch[pl.ds(place * sources + me, 1), :] for place in range(4)
        )
        ideal_sum = jnp.zeros((1, LANES), jnp.float32)
        for query in range(2):
            asked = query + 1.0
            per_lane = jnp.sum(jnp.where(mark == asked, term, 0.0), axis=0, keepdims=True)
            spread = group_sum(jnp.broadcast_to(per_lane, (8, LANES)), capacity)[:1, :]
            ideal_sum = jnp.where(own_mark == asked, spread, ideal_sum)
        inv_ideal = jnp.where(ideal_sum > 0.0, 1.0 / jnp.where(ideal_sum > 0.0, ideal_sum, 1.0), 0.0)

        total = jnp.zeros((sources, LANES), jnp.float32)
        for c in range(capacity):
            at = slice(c * sources, (c + 1) * sources)
            their_gain = jnp.exp2(jnp.ceil(key_by[at, :] * (1.0 / slots))) - 1.0
            gain_gap = own_gain - their_gain
            gap = 2.0 * (score_by[at, :] - own_score)
            pull = jax.nn.sigmoid(jnp.where(gain_gap > 0.0, gap, -gap))
            pair = -gain_gap * jnp.abs(own_disc - disc_by[at, :]) * pull
            total = total + jnp.where(mark_by[at, :] == own_mark, pair, 0.0)
        lambda_row = jnp.sum(total, axis=0, keepdims=True) * inv_ideal
        here = slot_ref[...] == lane_of_row + h * LANES
        lambda_column = lambda_column + jnp.sum(
            jnp.where(here, lambda_row, 0.0), axis=1, keepdims=True
        )

    column_ref[...] = lambda_column
    along = lax.broadcasted_iota(jnp.int32, (rows, rows), 1)
    down = lax.broadcasted_iota(jnp.int32, (rows, rows), 0)
    row = jnp.sum(jnp.where(along == down, lambda_column, 0.0), axis=0, keepdims=True)
    spread_ref[...] = jnp.broadcast_to(row[None], spread_ref.shape)


def slope_kernel(count, place_ref, w1_ref, w2_ref, *refs):
    emb_refs, (slope_ref, hidden_ref, part_ref) = refs[:count], refs[count:]
    wide = part_ref.shape[2]
    mine = pl.ds(pl.multiple_of(place_ref[1] // 2 * wide, LANES), wide)
    for i, emb_ref in enumerate(emb_refs):
        pre_act = jnp.dot(emb_ref[...], w1_ref[...], preferred_element_type=jnp.float32)
        gate = jax.nn.sigmoid(pre_act)
        hidden_ref[i] = (pre_act * gate).astype(jnp.bfloat16)
        slope = gate * (1.0 + pre_act * (1.0 - gate))
        slope_ref[i] = (w2_ref[...] * slope).astype(jnp.bfloat16)
        part_ref[i] = emb_ref[:, mine]


def slopes(place, w_first, w2_row, blocks, wide):
    rows, units = blocks[0].shape[0], w_first.shape[1]
    count = len(blocks)
    return pl.pallas_call(
        functools.partial(slope_kernel, count),
        out_shape=(
            whole((count, rows, units), jnp.bfloat16),
            whole((count, rows, units), jnp.bfloat16),
            whole((count, rows, wide), jnp.bfloat16),
        ),
        in_specs=[pl.BlockSpec(memory_space=pltpu.SMEM)] + vmem_specs(2 + count),
        out_specs=tuple(vmem_specs(3)),
        name="slopes",
    )(place, w_first, w2_row, *blocks)


def product_kernel(groups, place_ref, lambda_ref, *refs):
    inputs, sent_ref = refs[: 3 * len(groups)], refs[-1]
    members, rows = lambda_ref.shape[0], lambda_ref.shape[2]
    my_member = place_ref[1] // 2
    along = lax.broadcasted_iota(jnp.int32, (rows, rows), 1)
    down = lax.broadcasted_iota(jnp.int32, (rows, rows), 0)
    total, second = None, None
    for g, offsets in enumerate(groups):
        slope_ref, hidden_ref, part_ref = inputs[3 * g : 3 * g + 3]
        for i, offset in enumerate(offsets):
            block = lambda_ref[lax.rem(my_member + offset, members)]
            column = jnp.sum(jnp.where(along == down, block[:1], 0.0), axis=1, keepdims=True)
            part = (part_ref[i].astype(jnp.float32) * column).astype(jnp.bfloat16)
            product = lax.dot_general(
                part, slope_ref[i], (((0,), (0,)), ((), ())), preferred_element_type=jnp.float32
            )
            high = block.astype(jnp.bfloat16)
            low = (block - high.astype(jnp.float32)).astype(jnp.bfloat16)
            hidden = hidden_ref[i]
            summed = jnp.dot(high, hidden, preferred_element_type=jnp.float32) + jnp.dot(
                low, hidden, preferred_element_type=jnp.float32
            )
            total = product if total is None else total + product
            second = summed if second is None else second + summed
    targets = sent_ref.shape[0]
    part_rows = total.shape[0] // targets
    columns = total.shape[1] // LANES
    rounded, second = total.astype(jnp.bfloat16), second.astype(jnp.bfloat16)
    for target in range(targets):
        for k in range(columns):
            at = slice(k * LANES, (k + 1) * LANES)
            sent_ref[target, k * part_rows : (k + 1) * part_rows, :] = rounded[
                target * part_rows : (target + 1) * part_rows, at
            ]
            row = part_rows * columns + k
            sent_ref[target, row : row + 1, :] = second[:1, at]


def sent_to_all(x, axis):
    count = lax.axis_size(axis)
    return lax.all_to_all(jnp.broadcast_to(x[None], (count, *x.shape)), axis, 0, 0, tiled=True)


def parity_blocks(block):
    lanes, subs = lax.axis_size("mp"), lax.axis_size("sub")

    def moved(x, by):
        return lax.ppermute(x, "mp", [(i, (i + by) % lanes) for i in range(lanes)])

    back, on = moved(block, 2), moved(block, -2)
    both_ways = [
        (i * subs + s, (i + (2 if s == 0 else -2)) % lanes * subs + s)
        for i in range(lanes)
        for s in range(subs)
    ]
    passed = jnp.where(lax.axis_index("sub") == 0, back, on)
    across = lax.ppermute(passed, ("mp", "sub"), both_ways)
    return back, on, across


def on_device(embeddings, owner_shard, query_local, labels, w_first, w_second):
    docs, lanes, subs = (lax.axis_size(axis) for axis in ("docs", "mp", "sub"))
    rows, width = embeddings.shape
    units = w_first.shape[1]
    capacity = 2 * rows // docs
    halves = docs * capacity // LANES
    w2_row = w_second.reshape(1, units)
    place = jnp.stack([lax.axis_index(axis) for axis in ("docs", "mp", "sub")]).astype(jnp.int32)
    back, on, across = parity_blocks(embeddings)
    members = lanes // 2
    sent, slot = pl.pallas_call(
        functools.partial(score_kernel, capacity),
        out_shape=(
            whole((docs, 4 * halves, LANES), jnp.float32),
            whole((rows, 1), jnp.int32),
        ),
        in_specs=vmem_specs(6),
        out_specs=tuple(vmem_specs(2)),
        name="score",
    )(
        embeddings, w_first, w2_row,
        owner_shard.reshape(1, rows), query_local.reshape(1, rows), labels.reshape(1, rows),
    )
    got = lax.all_to_all(sent, "docs", 0, 0, tiled=True)
    spread, lambda_column = pl.pallas_call(
        functools.partial(lambda_kernel, capacity),
        out_shape=(whole((members, 8, rows), jnp.float32), whole((rows, 1), jnp.float32)),
        in_specs=[pl.BlockSpec(memory_space=pltpu.SMEM)] + vmem_specs(2),
        out_specs=tuple(vmem_specs(2)),
        scratch_shapes=[pltpu.VMEM((docs * capacity, LANES), jnp.float32)] * 4
        + [pltpu.VMEM((4 * docs, LANES), jnp.float32)],
        name="lambdas",
    )(place, got, slot)
    parities = [list(range(parity, lanes, 2)) for parity in range(2)]
    all_lambdas = lax.all_to_all(
        spread, "mp", 0, 0, axis_index_groups=parities, tiled=True
    )

    part_rows = width // (lanes * subs)
    targets = 2 * subs
    wide = targets * part_rows
    columns = units // LANES
    own = slopes(place, w_first, w2_row, [embeddings], wide)
    beside = slopes(place, w_first, w2_row, [back, on], wide)
    beyond = slopes(place, w_first, w2_row, [across], wide)
    own_grad = lax.dot_general(
        own[0][0], w_first, (((1,), (1,)), ((), ())), preferred_element_type=jnp.float32
    )
    emb_grad = (lambda_column * own_grad).astype(jnp.bfloat16)
    all_lambdas, emb_grad = lax.optimization_barrier((all_lambdas, emb_grad))
    offsets = ((0,), (members - 1, 1), (2,))
    sent = pl.pallas_call(
        functools.partial(product_kernel, offsets),
        out_shape=whole((targets, (part_rows + 1) * columns, LANES), jnp.bfloat16),
        in_specs=[pl.BlockSpec(memory_space=pltpu.SMEM)] + vmem_specs(10),
        out_specs=vmem_specs(1)[0],
        name="product",
    )(place, all_lambdas, *own, *beside, *beyond)
    cells = [list(range(i, i + targets)) for i in range(0, lanes * subs, targets)]
    arrived = lax.all_to_all(
        sent, ("mp", "sub"), 0, 0, axis_index_groups=cells, tiled=True
    )
    line_sum = arrived.astype(jnp.float32).sum(axis=0).astype(jnp.bfloat16)
    first_rows = part_rows * columns
    tiles = line_sum[:first_rows].reshape(docs, first_rows // docs, LANES)
    second = jnp.broadcast_to(line_sum[first_rows:][None], (docs, columns, LANES))
    arrived = lax.all_to_all(jnp.concatenate([tiles, second], axis=1), "docs", 0, 0, tiled=True)
    shard_sum = arrived.astype(jnp.float32).sum(axis=0)
    w_second_grad = shard_sum[first_rows // docs :].reshape(units)
    spread = sent_to_all(shard_sum[: first_rows // docs].astype(jnp.bfloat16), "docs")
    w_first_grad = (
        spread.reshape(columns, part_rows, LANES).transpose(1, 0, 2).reshape(part_rows, units)
    ).astype(jnp.float32)
    return (emb_grad, w_first_grad, w_second_grad)


def solution(mesh):
    split = ("groups", "docs", "mp", "sub")
    return jax.shard_map(
        on_device,
        mesh=mesh,
        in_specs=(P(split, None), P(split, None), P(split), P(split), P(), P()),
        out_specs=(P(split, None), P(("groups", "mp", "sub"), None), P("groups")),
        check_vma=False,
    )
```

```python
import functools

import jax
import jax.numpy as jnp
from jax import lax
from jax.experimental import pallas as pl
from jax.experimental.pallas import tpu as pltpu
from jax.sharding import PartitionSpec as P


LANES = 128


def whole(*shape_and_type):
    return jax.ShapeDtypeStruct(*shape_and_type)


def vmem_specs(count):
    return [pl.BlockSpec(memory_space=pltpu.VMEM)] * count


def score_kernel(capacity, emb_ref, w1_ref, w2_ref, owner_ref, query_ref, label_ref, sent_ref, slot_ref):
    rows = emb_ref.shape[0]
    halves = sent_ref.shape[1] // 4
    along = lax.broadcasted_iota(jnp.int32, (rows, rows), 1)
    down = lax.broadcasted_iota(jnp.int32, (rows, rows), 0)

    def column(row):
        return jnp.sum(jnp.where(along == down, row, 0), axis=1, keepdims=True)

    owner = owner_ref[...]
    owner_column = column(owner)
    earlier = jnp.where((owner_column == owner) & (along < down), 1, 0)
    slot = owner_column * capacity + jnp.sum(earlier, axis=1, keepdims=True)
    slot_ref[...] = slot
    mark = column(query_ref[...] + 1).astype(jnp.float32)
    label = column(label_ref[...]).astype(jnp.float32)

    pre_act = jnp.dot(emb_ref[...], w1_ref[...], preferred_element_type=jnp.float32)
    hidden = pre_act * jax.nn.sigmoid(pre_act)
    score = jnp.sum(hidden * w2_ref[...], axis=1, keepdims=True)

    lane = lax.broadcasted_iota(jnp.int32, (rows, LANES), 1)
    sent_ref[...] = jnp.zeros_like(sent_ref)
    for h in range(halves):
        here = slot == lane + h * LANES
        for place, value in enumerate((score, mark, label)):
            row = jnp.sum(jnp.where(here, value, 0.0), axis=0, keepdims=True)
            for target in range(sent_ref.shape[0]):
                sent_ref[target, place * halves + h : place * halves + h + 1, :] = row


def within_groups(x, capacity):
    lane = lax.broadcasted_iota(jnp.int32, x.shape, 1)
    out = [x]
    step = capacity // 2
    while step:
        upper = (lane & step) != 0
        spread = []
        for y in out:
            spread.append(jnp.where(upper, pltpu.roll(y, step, 1), y))
            spread.append(jnp.where(upper, y, pltpu.roll(y, LANES - step, 1)))
        out = spread
        step //= 2
    return out


def group_sum(x, capacity):
    lane = lax.broadcasted_iota(jnp.int32, x.shape, 1)
    step = capacity // 2
    while step:
        upper = (lane & step) != 0
        x = x + jnp.where(upper, pltpu.roll(x, step, 1), pltpu.roll(x, LANES - step, 1))
        step //= 2
    return x


def lambda_kernel(
    capacity, place_ref, got_ref, slot_ref, spread_ref, column_ref,
    score_by, mark_by, key_by, disc_by, row_scratch,
):
    sources = got_ref.shape[0]
    halves = got_ref.shape[1] // 4
    me = place_ref[0]
    rows = slot_ref.shape[0]
    source = lax.broadcasted_iota(jnp.int32, (sources, LANES), 0)
    lane = lax.broadcasted_iota(jnp.int32, (sources, LANES), 1)
    position = (source * capacity + lane % capacity).astype(jnp.float32)
    slots = float(sources * capacity)
    lane_of_row = lax.broadcasted_iota(jnp.int32, (rows, LANES), 1)
    lambda_column = jnp.zeros((rows, 1), jnp.float32)
    for h in range(halves):
        half_score = got_ref[:, h, :] * 0.5
        mark = got_ref[:, halves + h, :]
        label = got_ref[:, 2 * halves + h, :]
        key = label * slots - position
        for ref, value in ((score_by, half_score), (mark_by, mark), (key_by, key)):
            for c, spread in enumerate(within_groups(value, capacity)):
                ref[c * sources : (c + 1) * sources, :] = spread

        def rank_step(step, sums):
            soft, ideal = sums
            base = pl.multiple_of(step * 8, 8)
            score_rows = score_by[pl.ds(base, 8), :]
            mark_rows = mark_by[pl.ds(base, 8), :]
            key_rows = key_by[pl.ds(base, 8), :]
            for r in range(8):
                same = mark_rows[r : r + 1, :] == mark
                tilt = jnp.tanh(score_rows[r : r + 1, :] - half_score)
                soft = soft + jnp.where(same, tilt + 1.0, 0.0)
                ideal = ideal + jnp.where(same & (key_rows[r : r + 1, :] > key), 1.0, 0.0)
            return soft, ideal

        nothing = jnp.zeros((sources, LANES), jnp.float32)
        soft, ideal = lax.fori_loop(0, capacity * sources // 8, rank_step, (nothing, nothing))
        discount = 1.0 / jnp.log2(2.0 + (0.5 * soft - 0.5))
        gain = jnp.exp2(label) - 1.0
        term = gain / jnp.log2(2.0 + ideal)
        for c, spread in enumerate(within_groups(discount, capacity)):
            disc_by[c * sources : (c + 1) * sources, :] = spread

        for place, value in enumerate((half_score, mark, gain, discount)):
            row_scratch[place * sources : (place + 1) * sources, :] = value
        own_score, own_mark, own_gain, own_disc = (
            row_scratch[pl.ds(place * sources + me, 1), :] for place in range(4)
        )
        ideal_sum = jnp.zeros((1, LANES), jnp.float32)
        for query in range(2):
            asked = query + 1.0
            per_lane = jnp.sum(jnp.where(mark == asked, term, 0.0), axis=0, keepdims=True)
            spread = group_sum(jnp.broadcast_to(per_lane, (8, LANES)), capacity)[:1, :]
            ideal_sum = jnp.where(own_mark == asked, spread, ideal_sum)
        inv_ideal = jnp.where(ideal_sum > 0.0, 1.0 / jnp.where(ideal_sum > 0.0, ideal_sum, 1.0), 0.0)

        total = jnp.zeros((sources, LANES), jnp.float32)
        for c in range(capacity):
            at = slice(c * sources, (c + 1) * sources)
            their_gain = jnp.exp2(jnp.ceil(key_by[at, :] * (1.0 / slots))) - 1.0
            gain_gap = own_gain - their_gain
            gap = 2.0 * (score_by[at, :] - own_score)
            pull = jax.nn.sigmoid(jnp.where(gain_gap > 0.0, gap, -gap))
            pair = -gain_gap * jnp.abs(own_disc - disc_by[at, :]) * pull
            total = total + jnp.where(mark_by[at, :] == own_mark, pair, 0.0)
        lambda_row = jnp.sum(total, axis=0, keepdims=True) * inv_ideal
        here = slot_ref[...] == lane_of_row + h * LANES
        lambda_column = lambda_column + jnp.sum(
            jnp.where(here, lambda_row, 0.0), axis=1, keepdims=True
        )

    column_ref[...] = lambda_column
    along = lax.broadcasted_iota(jnp.int32, (rows, rows), 1)
    down = lax.broadcasted_iota(jnp.int32, (rows, rows), 0)
    row = jnp.sum(jnp.where(along == down, lambda_column, 0.0), axis=0, keepdims=True)
    spread_ref[...] = jnp.broadcast_to(row[None], spread_ref.shape)


def slope_kernel(count, place_ref, w1_ref, w2_ref, *refs):
    emb_refs, (slope_ref, hidden_ref, part_ref) = refs[:count], refs[count:]
    wide = part_ref.shape[2]
    mine = pl.ds(pl.multiple_of(place_ref[1] // 2 * wide, LANES), wide)
    for i, emb_ref in enumerate(emb_refs):
        pre_act = jnp.dot(emb_ref[...], w1_ref[...], preferred_element_type=jnp.float32)
        gate = jax.nn.sigmoid(pre_act)
        hidden_ref[i] = (pre_act * gate).astype(jnp.bfloat16)
        slope = gate * (1.0 + pre_act * (1.0 - gate))
        slope_ref[i] = (w2_ref[...] * slope).astype(jnp.bfloat16)
        part_ref[i] = emb_ref[:, mine]


def slopes(place, w_first, w2_row, blocks, wide):
    rows, units = blocks[0].shape[0], w_first.shape[1]
    count = len(blocks)
    return pl.pallas_call(
        functools.partial(slope_kernel, count),
        out_shape=(
            whole((count, rows, units), jnp.bfloat16),
            whole((count, rows, units), jnp.bfloat16),
            whole((count, rows, wide), jnp.bfloat16),
        ),
        in_specs=[pl.BlockSpec(memory_space=pltpu.SMEM)] + vmem_specs(2 + count),
        out_specs=tuple(vmem_specs(3)),
        name="slopes",
    )(place, w_first, w2_row, *blocks)


def product_kernel(groups, place_ref, lambda_ref, *refs):
    inputs, sent_ref = refs[: 3 * len(groups)], refs[-1]
    members, rows = lambda_ref.shape[0], lambda_ref.shape[2]
    my_member = place_ref[1] // 2
    along = lax.broadcasted_iota(jnp.int32, (rows, rows), 1)
    down = lax.broadcasted_iota(jnp.int32, (rows, rows), 0)
    total, second = None, None
    for g, offsets in enumerate(groups):
        slope_ref, hidden_ref, part_ref = inputs[3 * g : 3 * g + 3]
        for i, offset in enumerate(offsets):
            block = lambda_ref[lax.rem(my_member + offset, members)]
            column = jnp.sum(jnp.where(along == down, block[:1], 0.0), axis=1, keepdims=True)
            part = (part_ref[i].astype(jnp.float32) * column).astype(jnp.bfloat16)
            product = lax.dot_general(
                part, slope_ref[i], (((0,), (0,)), ((), ())), preferred_element_type=jnp.float32
            )
            high = block.astype(jnp.bfloat16)
            low = (block - high.astype(jnp.float32)).astype(jnp.bfloat16)
            hidden = hidden_ref[i]
            summed = jnp.dot(high, hidden, preferred_element_type=jnp.float32) + jnp.dot(
                low, hidden, preferred_element_type=jnp.float32
            )
            total = product if total is None else total + product
            second = summed if second is None else second + summed
    targets = sent_ref.shape[0]
    part_rows = total.shape[0] // targets
    columns = total.shape[1] // LANES
    rounded, second = total.astype(jnp.bfloat16), second.astype(jnp.bfloat16)
    for target in range(targets):
        for k in range(columns):
            at = slice(k * LANES, (k + 1) * LANES)
            sent_ref[target, k * part_rows : (k + 1) * part_rows, :] = rounded[
                target * part_rows : (target + 1) * part_rows, at
            ]
            row = part_rows * columns + k
            sent_ref[target, row : row + 1, :] = second[:1, at]


def sent_to_all(x, axis):
    count = lax.axis_size(axis)
    return lax.all_to_all(jnp.broadcast_to(x[None], (count, *x.shape)), axis, 0, 0, tiled=True)


def parity_blocks(block):
    lanes, subs = lax.axis_size("mp"), lax.axis_size("sub")

    def moved(x, by):
        return lax.ppermute(x, "mp", [(i, (i + by) % lanes) for i in range(lanes)])

    back, on = moved(block, 2), moved(block, -2)
    both_ways = [
        (i * subs + s, (i + (2 if s == 0 else -2)) % lanes * subs + s)
        for i in range(lanes)
        for s in range(subs)
    ]
    passed = jnp.where(lax.axis_index("sub") == 0, back, on)
    across = lax.ppermute(passed, ("mp", "sub"), both_ways)
    return back, on, across


def on_device(embeddings, owner_shard, query_local, labels, w_first, w_second):
    docs, lanes, subs = (lax.axis_size(axis) for axis in ("docs", "mp", "sub"))
    rows, width = embeddings.shape
    units = w_first.shape[1]
    capacity = 2 * rows // docs
    halves = docs * capacity // LANES
    w2_row = w_second.reshape(1, units)
    place = jnp.stack([lax.axis_index(axis) for axis in ("docs", "mp", "sub")]).astype(jnp.int32)
    back, on, across = parity_blocks(embeddings)
    members = lanes // 2
    sent, slot = pl.pallas_call(
        functools.partial(score_kernel, capacity),
        out_shape=(
            whole((docs, 4 * halves, LANES), jnp.float32),
            whole((rows, 1), jnp.int32),
        ),
        in_specs=vmem_specs(6),
        out_specs=tuple(vmem_specs(2)),
        name="score",
    )(
        embeddings, w_first, w2_row,
        owner_shard.reshape(1, rows), query_local.reshape(1, rows), labels.reshape(1, rows),
    )
    got = lax.all_to_all(sent, "docs", 0, 0, tiled=True)
    spread, lambda_column = pl.pallas_call(
        functools.partial(lambda_kernel, capacity),
        out_shape=(whole((members, 8, rows), jnp.float32), whole((rows, 1), jnp.float32)),
        in_specs=[pl.BlockSpec(memory_space=pltpu.SMEM)] + vmem_specs(2),
        out_specs=tuple(vmem_specs(2)),
        scratch_shapes=[pltpu.VMEM((docs * capacity, LANES), jnp.float32)] * 4
        + [pltpu.VMEM((4 * docs, LANES), jnp.float32)],
        name="lambdas",
    )(place, got, slot)
    parities = [list(range(parity, lanes, 2)) for parity in range(2)]
    all_lambdas = lax.all_to_all(
        spread, "mp", 0, 0, axis_index_groups=parities, tiled=True
    )

    part_rows = width // (lanes * subs)
    targets = 2 * subs
    wide = targets * part_rows
    columns = units // LANES
    prepared = slopes(place, w_first, w2_row, [embeddings, back, on, across], wide)
    offsets = ((0, members - 1, 1, 2),)
    sent = pl.pallas_call(
        functools.partial(product_kernel, offsets),
        out_shape=whole((targets, (part_rows + 1) * columns, LANES), jnp.bfloat16),
        in_specs=[pl.BlockSpec(memory_space=pltpu.SMEM)] + vmem_specs(4),
        out_specs=vmem_specs(1)[0],
        name="product",
    )(place, all_lambdas, *prepared)
    cells = [list(range(i, i + targets)) for i in range(0, lanes * subs, targets)]
    arrived = lax.all_to_all(
        sent, ("mp", "sub"), 0, 0, axis_index_groups=cells, tiled=True
    )
    line_sum = arrived.astype(jnp.float32).sum(axis=0).astype(jnp.bfloat16)
    first_rows = part_rows * columns
    tiles = line_sum[:first_rows].reshape(docs, first_rows // docs, LANES)
    second = jnp.broadcast_to(line_sum[first_rows:][None], (docs, columns, LANES))
    arrived = lax.all_to_all(jnp.concatenate([tiles, second], axis=1), "docs", 0, 0, tiled=True)
    shard_sum = arrived.astype(jnp.float32).sum(axis=0)
    lambda_column, shard_sum = lax.optimization_barrier((lambda_column, shard_sum))
    own_grad = lax.dot_general(
        prepared[0][0], w_first, (((1,), (1,)), ((), ())), preferred_element_type=jnp.float32
    )
    emb_grad = (lambda_column * own_grad).astype(jnp.bfloat16)
    w_second_grad = shard_sum[first_rows // docs :].reshape(units)
    spread = sent_to_all(shard_sum[: first_rows // docs].astype(jnp.bfloat16), "docs")
    w_first_grad = (
        spread.reshape(columns, part_rows, LANES).transpose(1, 0, 2).reshape(part_rows, units)
    ).astype(jnp.float32)
    return (emb_grad, w_first_grad, w_second_grad)


def solution(mesh):
    split = ("groups", "docs", "mp", "sub")
    return jax.shard_map(
        on_device,
        mesh=mesh,
        in_specs=(P(split, None), P(split, None), P(split), P(split), P(), P()),
        out_specs=(P(split, None), P(("groups", "mp", "sub"), None), P("groups")),
        check_vma=False,
    )
```

```python
import functools

import jax
import jax.numpy as jnp
from jax import lax
from jax.experimental import pallas as pl
from jax.experimental.pallas import tpu as pltpu
from jax.sharding import PartitionSpec as P


LANES = 128


def whole(*shape_and_type):
    return jax.ShapeDtypeStruct(*shape_and_type)


def vmem_specs(count):
    return [pl.BlockSpec(memory_space=pltpu.VMEM)] * count


def score_kernel(capacity, emb_ref, w1_ref, w2_ref, owner_ref, query_ref, label_ref, sent_ref, slot_ref):
    rows = emb_ref.shape[0]
    halves = sent_ref.shape[1] // 4
    along = lax.broadcasted_iota(jnp.int32, (rows, rows), 1)
    down = lax.broadcasted_iota(jnp.int32, (rows, rows), 0)

    def column(row):
        return jnp.sum(jnp.where(along == down, row, 0), axis=1, keepdims=True)

    owner = owner_ref[...]
    owner_column = column(owner)
    earlier = jnp.where((owner_column == owner) & (along < down), 1, 0)
    slot = owner_column * capacity + jnp.sum(earlier, axis=1, keepdims=True)
    slot_ref[...] = slot
    mark = column(query_ref[...] + 1).astype(jnp.float32)
    label = column(label_ref[...]).astype(jnp.float32)

    pre_act = jnp.dot(emb_ref[...], w1_ref[...], preferred_element_type=jnp.float32)
    hidden = pre_act * jax.nn.sigmoid(pre_act)
    score = jnp.sum(hidden * w2_ref[...], axis=1, keepdims=True)

    lane = lax.broadcasted_iota(jnp.int32, (rows, LANES), 1)
    sent_ref[...] = jnp.zeros_like(sent_ref)
    for h in range(halves):
        here = slot == lane + h * LANES
        for place, value in enumerate((score, mark, label)):
            row = jnp.sum(jnp.where(here, value, 0.0), axis=0, keepdims=True)
            for target in range(sent_ref.shape[0]):
                sent_ref[target, place * halves + h : place * halves + h + 1, :] = row


def within_groups(x, capacity):
    lane = lax.broadcasted_iota(jnp.int32, x.shape, 1)
    out = [x]
    step = capacity // 2
    while step:
        upper = (lane & step) != 0
        spread = []
        for y in out:
            spread.append(jnp.where(upper, pltpu.roll(y, step, 1), y))
            spread.append(jnp.where(upper, y, pltpu.roll(y, LANES - step, 1)))
        out = spread
        step //= 2
    return out


def group_sum(x, capacity):
    lane = lax.broadcasted_iota(jnp.int32, x.shape, 1)
    step = capacity // 2
    while step:
        upper = (lane & step) != 0
        x = x + jnp.where(upper, pltpu.roll(x, step, 1), pltpu.roll(x, LANES - step, 1))
        step //= 2
    return x


def lambda_kernel(
    capacity, place_ref, got_ref, slot_ref, spread_ref, column_ref,
    score_by, mark_by, key_by, disc_by, row_scratch,
):
    sources = got_ref.shape[0]
    halves = got_ref.shape[1] // 4
    me = place_ref[0]
    rows = slot_ref.shape[0]
    source = lax.broadcasted_iota(jnp.int32, (sources, LANES), 0)
    lane = lax.broadcasted_iota(jnp.int32, (sources, LANES), 1)
    position = (source * capacity + lane % capacity).astype(jnp.float32)
    slots = float(sources * capacity)
    lane_of_row = lax.broadcasted_iota(jnp.int32, (rows, LANES), 1)
    lambda_column = jnp.zeros((rows, 1), jnp.float32)
    for h in range(halves):
        half_score = got_ref[:, h, :] * 0.5
        mark = got_ref[:, halves + h, :]
        label = got_ref[:, 2 * halves + h, :]
        key = label * slots - position
        for ref, value in ((score_by, half_score), (mark_by, mark), (key_by, key)):
            for c, spread in enumerate(within_groups(value, capacity)):
                ref[c * sources : (c + 1) * sources, :] = spread

        def rank_step(step, sums):
            soft, ideal = sums
            base = pl.multiple_of(step * 8, 8)
            score_rows = score_by[pl.ds(base, 8), :]
            mark_rows = mark_by[pl.ds(base, 8), :]
            key_rows = key_by[pl.ds(base, 8), :]
            for r in range(8):
                same = mark_rows[r : r + 1, :] == mark
                tilt = jnp.tanh(score_rows[r : r + 1, :] - half_score)
                soft = soft + jnp.where(same, tilt + 1.0, 0.0)
                ideal = ideal + jnp.where(same & (key_rows[r : r + 1, :] > key), 1.0, 0.0)
            return soft, ideal

        nothing = jnp.zeros((sources, LANES), jnp.float32)
        soft, ideal = lax.fori_loop(0, capacity * sources // 8, rank_step, (nothing, nothing))
        discount = 1.0 / jnp.log2(2.0 + (0.5 * soft - 0.5))
        gain = jnp.exp2(label) - 1.0
        term = gain / jnp.log2(2.0 + ideal)
        for c, spread in enumerate(within_groups(discount, capacity)):
            disc_by[c * sources : (c + 1) * sources, :] = spread

        for place, value in enumerate((half_score, mark, gain, discount)):
            row_scratch[place * sources : (place + 1) * sources, :] = value
        own_score, own_mark, own_gain, own_disc = (
            row_scratch[pl.ds(place * sources + me, 1), :] for place in range(4)
        )
        ideal_sum = jnp.zeros((1, LANES), jnp.float32)
        for query in range(2):
            asked = query + 1.0
            per_lane = jnp.sum(jnp.where(mark == asked, term, 0.0), axis=0, keepdims=True)
            spread = group_sum(jnp.broadcast_to(per_lane, (8, LANES)), capacity)[:1, :]
            ideal_sum = jnp.where(own_mark == asked, spread, ideal_sum)
        inv_ideal = jnp.where(ideal_sum > 0.0, 1.0 / jnp.where(ideal_sum > 0.0, ideal_sum, 1.0), 0.0)

        total = jnp.zeros((sources, LANES), jnp.float32)
        for c in range(capacity):
            at = slice(c * sources, (c + 1) * sources)
            their_gain = jnp.exp2(jnp.ceil(key_by[at, :] * (1.0 / slots))) - 1.0
            gain_gap = own_gain - their_gain
            gap = 2.0 * (score_by[at, :] - own_score)
            pull = jax.nn.sigmoid(jnp.where(gain_gap > 0.0, gap, -gap))
            pair = -gain_gap * jnp.abs(own_disc - disc_by[at, :]) * pull
            total = total + jnp.where(mark_by[at, :] == own_mark, pair, 0.0)
        lambda_row = jnp.sum(total, axis=0, keepdims=True) * inv_ideal
        here = slot_ref[...] == lane_of_row + h * LANES
        lambda_column = lambda_column + jnp.sum(
            jnp.where(here, lambda_row, 0.0), axis=1, keepdims=True
        )

    column_ref[...] = lambda_column
    along = lax.broadcasted_iota(jnp.int32, (rows, rows), 1)
    down = lax.broadcasted_iota(jnp.int32, (rows, rows), 0)
    row = jnp.sum(jnp.where(along == down, lambda_column, 0.0), axis=0, keepdims=True)
    spread_ref[...] = jnp.broadcast_to(row[None], spread_ref.shape)


def slope_kernel(count, place_ref, w1_ref, w2_ref, *refs):
    emb_refs, (slope_ref, hidden_ref, part_ref) = refs[:count], refs[count:]
    wide = part_ref.shape[2]
    mine = pl.ds(pl.multiple_of(place_ref[1] // 2 * wide, LANES), wide)
    for i, emb_ref in enumerate(emb_refs):
        pre_act = jnp.dot(emb_ref[...], w1_ref[...], preferred_element_type=jnp.float32)
        gate = jax.nn.sigmoid(pre_act)
        hidden_ref[i] = (pre_act * gate).astype(jnp.bfloat16)
        slope = gate * (1.0 + pre_act * (1.0 - gate))
        slope_ref[i] = (w2_ref[...] * slope).astype(jnp.bfloat16)
        part_ref[i] = emb_ref[:, mine]


def slopes(place, w_first, w2_row, blocks, wide):
    rows, units = blocks[0].shape[0], w_first.shape[1]
    count = len(blocks)
    return pl.pallas_call(
        functools.partial(slope_kernel, count),
        out_shape=(
            whole((count, rows, units), jnp.bfloat16),
            whole((count, rows, units), jnp.bfloat16),
            whole((count, rows, wide), jnp.bfloat16),
        ),
        in_specs=[pl.BlockSpec(memory_space=pltpu.SMEM)] + vmem_specs(2 + count),
        out_specs=tuple(vmem_specs(3)),
        name="slopes",
    )(place, w_first, w2_row, *blocks)


def product_kernel(groups, place_ref, lambda_ref, *refs):
    inputs, sent_ref = refs[: 3 * len(groups)], refs[-1]
    members, rows = lambda_ref.shape[0], lambda_ref.shape[2]
    my_member = place_ref[1] // 2
    along = lax.broadcasted_iota(jnp.int32, (rows, rows), 1)
    down = lax.broadcasted_iota(jnp.int32, (rows, rows), 0)
    total, second = None, None
    for g, offsets in enumerate(groups):
        slope_ref, hidden_ref, part_ref = inputs[3 * g : 3 * g + 3]
        for i, offset in enumerate(offsets):
            block = lambda_ref[lax.rem(my_member + offset, members)]
            column = jnp.sum(jnp.where(along == down, block[:1], 0.0), axis=1, keepdims=True)
            part = (part_ref[i].astype(jnp.float32) * column).astype(jnp.bfloat16)
            product = lax.dot_general(
                part, slope_ref[i], (((0,), (0,)), ((), ())), preferred_element_type=jnp.float32
            )
            high = block.astype(jnp.bfloat16)
            low = (block - high.astype(jnp.float32)).astype(jnp.bfloat16)
            hidden = hidden_ref[i]
            summed = jnp.dot(high, hidden, preferred_element_type=jnp.float32) + jnp.dot(
                low, hidden, preferred_element_type=jnp.float32
            )
            total = product if total is None else total + product
            second = summed if second is None else second + summed
    targets = sent_ref.shape[0]
    part_rows = total.shape[0] // targets
    columns = total.shape[1] // LANES
    rounded, second = total.astype(jnp.bfloat16), second.astype(jnp.bfloat16)
    for target in range(targets):
        for k in range(columns):
            at = slice(k * LANES, (k + 1) * LANES)
            sent_ref[target, k * part_rows : (k + 1) * part_rows, :] = rounded[
                target * part_rows : (target + 1) * part_rows, at
            ]
            row = part_rows * columns + k
            sent_ref[target, row : row + 1, :] = second[:1, at]


def docs_exchange(x):
    count = lax.axis_size("docs")
    members = [(i + count // 2) % count for i in range(count)]
    return lax.all_to_all(x, "docs", 0, 0, axis_index_groups=[members], tiled=True)


def parity_blocks(block):
    lanes, subs = lax.axis_size("mp"), lax.axis_size("sub")

    def moved(x, by):
        return lax.ppermute(x, "mp", [(i, (i + by) % lanes) for i in range(lanes)])

    back, on = moved(block, 2), moved(block, -2)
    both_ways = [
        (i * subs + s, (i + (2 if s == 0 else -2)) % lanes * subs + s)
        for i in range(lanes)
        for s in range(subs)
    ]
    passed = jnp.where(lax.axis_index("sub") == 0, back, on)
    across = lax.ppermute(passed, ("mp", "sub"), both_ways)
    return back, on, across


def on_device(embeddings, owner_shard, query_local, labels, w_first, w_second):
    docs, lanes, subs = (lax.axis_size(axis) for axis in ("docs", "mp", "sub"))
    rows, width = embeddings.shape
    units = w_first.shape[1]
    capacity = 2 * rows // docs
    halves = docs * capacity // LANES
    w2_row = w_second.reshape(1, units)
    place = jnp.stack([lax.axis_index(axis) for axis in ("docs", "mp", "sub")]).astype(jnp.int32)
    back, on, across = parity_blocks(embeddings)
    members = lanes // 2
    sent, slot = pl.pallas_call(
        functools.partial(score_kernel, capacity),
        out_shape=(
            whole((docs, 4 * halves, LANES), jnp.float32),
            whole((rows, 1), jnp.int32),
        ),
        in_specs=vmem_specs(6),
        out_specs=tuple(vmem_specs(2)),
        name="score",
    )(
        embeddings, w_first, w2_row,
        owner_shard.reshape(1, rows), query_local.reshape(1, rows), labels.reshape(1, rows),
    )
    got = lax.all_to_all(sent, "docs", 0, 0, tiled=True)
    spread, lambda_column = pl.pallas_call(
        functools.partial(lambda_kernel, capacity),
        out_shape=(whole((members, 8, rows), jnp.float32), whole((rows, 1), jnp.float32)),
        in_specs=[pl.BlockSpec(memory_space=pltpu.SMEM)] + vmem_specs(2),
        out_specs=tuple(vmem_specs(2)),
        scratch_shapes=[pltpu.VMEM((docs * capacity, LANES), jnp.float32)] * 4
        + [pltpu.VMEM((4 * docs, LANES), jnp.float32)],
        name="lambdas",
    )(place, got, slot)
    parities = [list(range(parity, lanes, 2)) for parity in range(2)]
    all_lambdas = lax.all_to_all(
        spread, "mp", 0, 0, axis_index_groups=parities, tiled=True
    )

    part_rows = width // (lanes * subs)
    targets = 2 * subs
    wide = targets * part_rows
    columns = units // LANES
    prepared = slopes(place, w_first, w2_row, [embeddings, back, on, across], wide)
    offsets = ((0, members - 1, 1, 2),)
    sent = pl.pallas_call(
        functools.partial(product_kernel, offsets),
        out_shape=whole((targets, (part_rows + 1) * columns, LANES), jnp.bfloat16),
        in_specs=[pl.BlockSpec(memory_space=pltpu.SMEM)] + vmem_specs(4),
        out_specs=vmem_specs(1)[0],
        name="product",
    )(place, all_lambdas, *prepared)
    cells = [list(range(i, i + targets)) for i in range(0, lanes * subs, targets)]
    arrived = lax.all_to_all(
        sent, ("mp", "sub"), 0, 0, axis_index_groups=cells, tiled=True
    )
    line_sum = arrived.astype(jnp.float32).sum(axis=0).astype(jnp.bfloat16)
    first_rows = part_rows * columns
    tiles = line_sum[:first_rows].reshape(docs, first_rows // docs, LANES)
    second = jnp.broadcast_to(line_sum[first_rows:][None], (docs, columns, LANES))
    arrived = docs_exchange(jnp.concatenate([tiles, second], axis=1))
    shard_sum = arrived.astype(jnp.float32).sum(axis=0)
    lambda_column, shard_sum = lax.optimization_barrier((lambda_column, shard_sum))
    own_grad = lax.dot_general(
        prepared[0][0], w_first, (((1,), (1,)), ((), ())), preferred_element_type=jnp.float32
    )
    emb_grad = (lambda_column * own_grad).astype(jnp.bfloat16)
    w_second_grad = shard_sum[first_rows // docs :].reshape(units)
    mine = shard_sum[: first_rows // docs].astype(jnp.bfloat16)
    spread = docs_exchange(jnp.broadcast_to(mine[None], (docs, *mine.shape)))
    w_first_grad = (
        spread.reshape(columns, part_rows, LANES).transpose(1, 0, 2).reshape(part_rows, units)
    ).astype(jnp.float32)
    return (emb_grad, w_first_grad, w_second_grad)


def solution(mesh):
    split = ("groups", "docs", "mp", "sub")
    return jax.shard_map(
        on_device,
        mesh=mesh,
        in_specs=(P(split, None), P(split, None), P(split), P(split), P(), P()),
        out_specs=(P(split, None), P(("groups", "mp", "sub"), None), P("groups")),
        check_vma=False,
    )
```

```python
import functools

import jax
import jax.numpy as jnp
from jax import lax
from jax.experimental import pallas as pl
from jax.experimental.pallas import tpu as pltpu
from jax.sharding import PartitionSpec as P


LANES = 128


def whole(*shape_and_type):
    return jax.ShapeDtypeStruct(*shape_and_type)


def on_chip(x):
    return pltpu.with_memory_space_constraint(x, pltpu.VMEM)


def vmem_specs(count):
    return [pl.BlockSpec(memory_space=pltpu.VMEM)] * count


def score_kernel(
    capacity, emb_ref, w1_ref, w2_ref, owner_ref, query_ref, label_ref, sent_ref, slot_ref, sum_ref
):
    rows = emb_ref.shape[0]
    targets, halves = sent_ref.shape[0], sent_ref.shape[1] // 4
    lane = lax.broadcasted_iota(jnp.int32, (rows, LANES), 1)

    def send(place, value):
        for h in range(halves):
            here = slot_ref[...] == lane + h * LANES
            row = jnp.sum(jnp.where(here, value, 0.0), axis=0, keepdims=True)
            for target in range(targets):
                sent_ref[target, place * halves + h : place * halves + h + 1, :] = row

    @pl.when(pl.program_id(0) == 0)
    def _():
        along = lax.broadcasted_iota(jnp.int32, (rows, rows), 1)
        down = lax.broadcasted_iota(jnp.int32, (rows, rows), 0)

        def column(row):
            return jnp.sum(jnp.where(along == down, row, 0), axis=1, keepdims=True)

        owner = owner_ref[...]
        owner_column = column(owner)
        earlier = jnp.where((owner_column == owner) & (along < down), 1, 0)
        slot_ref[...] = owner_column * capacity + jnp.sum(earlier, axis=1, keepdims=True)
        sum_ref[...] = jnp.zeros_like(sum_ref)
        sent_ref[...] = jnp.zeros_like(sent_ref)
        send(1, column(query_ref[...] + 1).astype(jnp.float32))
        send(2, column(label_ref[...]).astype(jnp.float32))

    pre_act = jnp.dot(emb_ref[...], w1_ref[...], preferred_element_type=jnp.float32)
    weighted = pre_act * jax.nn.sigmoid(pre_act) * w2_ref[...]
    part = sum_ref[...]
    for k in range(weighted.shape[1] // LANES):
        part = part + weighted[:, k * LANES : (k + 1) * LANES]
    sum_ref[...] = part

    @pl.when(pl.program_id(0) == pl.num_programs(0) - 1)
    def _():
        send(0, jnp.sum(sum_ref[...], axis=1, keepdims=True))


def within_groups(x, capacity):
    lane = lax.broadcasted_iota(jnp.int32, x.shape, 1)
    out = [x]
    step = capacity // 2
    while step:
        upper = (lane & step) != 0
        spread = []
        for y in out:
            spread.append(jnp.where(upper, pltpu.roll(y, step, 1), y))
            spread.append(jnp.where(upper, y, pltpu.roll(y, LANES - step, 1)))
        out = spread
        step //= 2
    return out


def group_sum(x, capacity):
    lane = lax.broadcasted_iota(jnp.int32, x.shape, 1)
    step = capacity // 2
    while step:
        upper = (lane & step) != 0
        x = x + jnp.where(upper, pltpu.roll(x, step, 1), pltpu.roll(x, LANES - step, 1))
        step //= 2
    return x


def lambda_kernel(
    capacity, place_ref, got_ref, slot_ref, spread_ref, column_ref,
    score_by, mark_by, key_by, disc_by, row_scratch,
):
    sources = got_ref.shape[0]
    halves = got_ref.shape[1] // 4
    me = place_ref[0]
    rows = slot_ref.shape[0]
    source = lax.broadcasted_iota(jnp.int32, (sources, LANES), 0)
    lane = lax.broadcasted_iota(jnp.int32, (sources, LANES), 1)
    position = (source * capacity + lane % capacity).astype(jnp.float32)
    slots = float(sources * capacity)
    lane_of_row = lax.broadcasted_iota(jnp.int32, (rows, LANES), 1)
    lambda_column = jnp.zeros((rows, 1), jnp.float32)
    for h in range(halves):
        half_score = got_ref[:, h, :] * 0.5
        mark = got_ref[:, halves + h, :]
        label = got_ref[:, 2 * halves + h, :]
        key = label * slots - position
        for ref, value in ((score_by, half_score), (mark_by, mark), (key_by, key)):
            for c, spread in enumerate(within_groups(value, capacity)):
                ref[c * sources : (c + 1) * sources, :] = spread

        def rank_step(step, sums):
            soft, ideal = sums
            base = pl.multiple_of(step * 8, 8)
            score_rows = score_by[pl.ds(base, 8), :]
            mark_rows = mark_by[pl.ds(base, 8), :]
            key_rows = key_by[pl.ds(base, 8), :]
            for r in range(8):
                same = mark_rows[r : r + 1, :] == mark
                tilt = jnp.tanh(score_rows[r : r + 1, :] - half_score)
                soft = soft + jnp.where(same, tilt + 1.0, 0.0)
                ideal = ideal + jnp.where(same & (key_rows[r : r + 1, :] > key), 1.0, 0.0)
            return soft, ideal

        nothing = jnp.zeros((sources, LANES), jnp.float32)
        soft, ideal = lax.fori_loop(0, capacity * sources // 8, rank_step, (nothing, nothing))
        discount = 1.0 / jnp.log2(2.0 + (0.5 * soft - 0.5))
        gain = jnp.exp2(label) - 1.0
        term = gain / jnp.log2(2.0 + ideal)
        for c, spread in enumerate(within_groups(discount, capacity)):
            disc_by[c * sources : (c + 1) * sources, :] = spread

        for place, value in enumerate((half_score, mark, gain, discount)):
            row_scratch[place * sources : (place + 1) * sources, :] = value
        own_score, own_mark, own_gain, own_disc = (
            row_scratch[pl.ds(place * sources + me, 1), :] for place in range(4)
        )
        ideal_sum = jnp.zeros((1, LANES), jnp.float32)
        for query in range(2):
            asked = query + 1.0
            per_lane = jnp.sum(jnp.where(mark == asked, term, 0.0), axis=0, keepdims=True)
            spread = group_sum(jnp.broadcast_to(per_lane, (8, LANES)), capacity)[:1, :]
            ideal_sum = jnp.where(own_mark == asked, spread, ideal_sum)
        inv_ideal = jnp.where(ideal_sum > 0.0, 1.0 / jnp.where(ideal_sum > 0.0, ideal_sum, 1.0), 0.0)

        total = jnp.zeros((sources, LANES), jnp.float32)
        for c in range(capacity):
            at = slice(c * sources, (c + 1) * sources)
            their_gain = jnp.exp2(jnp.ceil(key_by[at, :] * (1.0 / slots))) - 1.0
            gain_gap = own_gain - their_gain
            gap = 2.0 * (score_by[at, :] - own_score)
            pull = jax.nn.sigmoid(jnp.where(gain_gap > 0.0, gap, -gap))
            pair = -gain_gap * jnp.abs(own_disc - disc_by[at, :]) * pull
            total = total + jnp.where(mark_by[at, :] == own_mark, pair, 0.0)
        lambda_row = jnp.sum(total, axis=0, keepdims=True) * inv_ideal
        here = slot_ref[...] == lane_of_row + h * LANES
        lambda_column = lambda_column + jnp.sum(
            jnp.where(here, lambda_row, 0.0), axis=1, keepdims=True
        )

    column_ref[...] = lambda_column
    along = lax.broadcasted_iota(jnp.int32, (rows, rows), 1)
    down = lax.broadcasted_iota(jnp.int32, (rows, rows), 0)
    row = jnp.sum(jnp.where(along == down, lambda_column, 0.0), axis=0, keepdims=True)
    spread_ref[...] = jnp.broadcast_to(row[None], spread_ref.shape)


def slope_kernel(count, place_ref, w1_ref, w2_ref, *refs):
    emb_refs, (slope_ref, hidden_ref, part_ref) = refs[:count], refs[count:]
    wide = part_ref.shape[2]
    mine = pl.ds(pl.multiple_of(place_ref[1] // 2 * wide, LANES), wide)
    for i, emb_ref in enumerate(emb_refs):
        pre_act = jnp.dot(emb_ref[...], w1_ref[...], preferred_element_type=jnp.float32)
        gate = jax.nn.sigmoid(pre_act)
        hidden_ref[i] = (pre_act * gate).astype(jnp.bfloat16)
        slope = gate * (1.0 + pre_act * (1.0 - gate))
        slope_ref[i] = (w2_ref[...] * slope).astype(jnp.bfloat16)
        part_ref[i] = emb_ref[:, mine]


def slopes(place, w_first, w2_row, blocks, wide):
    rows, units = blocks[0].shape[0], w_first.shape[1]
    count = len(blocks)
    return pl.pallas_call(
        functools.partial(slope_kernel, count),
        out_shape=(
            whole((count, rows, units), jnp.bfloat16),
            whole((count, rows, units), jnp.bfloat16),
            whole((count, rows, wide), jnp.bfloat16),
        ),
        in_specs=[pl.BlockSpec(memory_space=pltpu.SMEM)] + vmem_specs(2 + count),
        out_specs=tuple(vmem_specs(3)),
        name="slopes",
    )(place, w_first, w2_row, *blocks)


def product_kernel(groups, place_ref, lambda_ref, *refs):
    inputs, sent_ref = refs[: 3 * len(groups)], refs[-1]
    members, rows = lambda_ref.shape[0], lambda_ref.shape[2]
    my_member = place_ref[1] // 2
    along = lax.broadcasted_iota(jnp.int32, (rows, rows), 1)
    down = lax.broadcasted_iota(jnp.int32, (rows, rows), 0)
    total, second = None, None
    for g, offsets in enumerate(groups):
        slope_ref, hidden_ref, part_ref = inputs[3 * g : 3 * g + 3]
        for i, offset in enumerate(offsets):
            block = lambda_ref[lax.rem(my_member + offset, members)]
            column = jnp.sum(jnp.where(along == down, block[:1], 0.0), axis=1, keepdims=True)
            part = (part_ref[i].astype(jnp.float32) * column).astype(jnp.bfloat16)
            product = lax.dot_general(
                part, slope_ref[i], (((0,), (0,)), ((), ())), preferred_element_type=jnp.float32
            )
            high = block.astype(jnp.bfloat16)
            low = (block - high.astype(jnp.float32)).astype(jnp.bfloat16)
            hidden = hidden_ref[i]
            summed = jnp.dot(high, hidden, preferred_element_type=jnp.float32) + jnp.dot(
                low, hidden, preferred_element_type=jnp.float32
            )
            total = product if total is None else total + product
            second = summed if second is None else second + summed
    targets = sent_ref.shape[0]
    part_rows = total.shape[0] // targets
    columns = total.shape[1] // LANES
    rounded, second = total.astype(jnp.bfloat16), second.astype(jnp.bfloat16)
    for target in range(targets):
        for k in range(columns):
            at = slice(k * LANES, (k + 1) * LANES)
            sent_ref[target, k * part_rows : (k + 1) * part_rows, :] = rounded[
                target * part_rows : (target + 1) * part_rows, at
            ]
            row = part_rows * columns + k
            sent_ref[target, row : row + 1, :] = second[:1, at]


def sent_to_all(x, axis):
    count = lax.axis_size(axis)
    return lax.all_to_all(jnp.broadcast_to(x[None], (count, *x.shape)), axis, 0, 0, tiled=True)


def parity_blocks(block):
    lanes, subs = lax.axis_size("mp"), lax.axis_size("sub")

    def moved(x, by):
        return lax.ppermute(x, "mp", [(i, (i + by) % lanes) for i in range(lanes)])

    back, on = moved(block, 2), moved(block, -2)
    both_ways = [
        (i * subs + s, (i + (2 if s == 0 else -2)) % lanes * subs + s)
        for i in range(lanes)
        for s in range(subs)
    ]
    passed = jnp.where(lax.axis_index("sub") == 0, back, on)
    across = lax.ppermute(passed, ("mp", "sub"), both_ways)
    return back, on, across


def on_device(embeddings, owner_shard, query_local, labels, w_first, w_second):
    docs, lanes, subs = (lax.axis_size(axis) for axis in ("docs", "mp", "sub"))
    rows, width = embeddings.shape
    units = w_first.shape[1]
    capacity = 2 * rows // docs
    halves = docs * capacity // LANES
    w2_row = w_second.reshape(1, units)
    place = jnp.stack([lax.axis_index(axis) for axis in ("docs", "mp", "sub")]).astype(jnp.int32)
    back, on, across = parity_blocks(embeddings)
    members = lanes // 2
    steps = 4

    def fixed(*shape):
        return pl.BlockSpec(shape, lambda j: (0,) * len(shape))

    sent, slot = pl.pallas_call(
        functools.partial(score_kernel, capacity),
        grid=(steps,),
        out_shape=(
            whole((docs, 4 * halves, LANES), jnp.float32),
            whole((rows, 1), jnp.int32),
        ),
        in_specs=[
            fixed(rows, width),
            pl.BlockSpec((width, units // steps), lambda j: (0, j)),
            pl.BlockSpec((1, units // steps), lambda j: (0, j)),
            fixed(1, rows),
            fixed(1, rows),
            fixed(1, rows),
        ],
        out_specs=(fixed(docs, 4 * halves, LANES), fixed(rows, 1)),
        scratch_shapes=[pltpu.VMEM((rows, LANES), jnp.float32)],
        name="score",
    )(
        embeddings, w_first, w2_row,
        owner_shard.reshape(1, rows), query_local.reshape(1, rows), labels.reshape(1, rows),
    )
    got = lax.all_to_all(sent, "docs", 0, 0, tiled=True)
    spread, lambda_column = pl.pallas_call(
        functools.partial(lambda_kernel, capacity),
        out_shape=(whole((members, 8, rows), jnp.float32), whole((rows, 1), jnp.float32)),
        in_specs=[pl.BlockSpec(memory_space=pltpu.SMEM)] + vmem_specs(2),
        out_specs=tuple(vmem_specs(2)),
        scratch_shapes=[pltpu.VMEM((docs * capacity, LANES), jnp.float32)] * 4
        + [pltpu.VMEM((4 * docs, LANES), jnp.float32)],
        name="lambdas",
    )(place, on_chip(got), slot)
    parities = [list(range(parity, lanes, 2)) for parity in range(2)]
    all_lambdas = lax.all_to_all(
        spread, "mp", 0, 0, axis_index_groups=parities, tiled=True
    )

    part_rows = width // (lanes * subs)
    targets = 2 * subs
    wide = targets * part_rows
    columns = units // LANES
    prepared = slopes(place, w_first, w2_row, [embeddings, back, on, across], wide)
    offsets = ((0, members - 1, 1, 2),)
    sent = pl.pallas_call(
        functools.partial(product_kernel, offsets),
        out_shape=pltpu.VMEM((targets, (part_rows + 1) * columns, LANES), jnp.bfloat16),
        in_specs=[pl.BlockSpec(memory_space=pltpu.SMEM)] + vmem_specs(4),
        out_specs=vmem_specs(1)[0],
        name="product",
    )(place, on_chip(all_lambdas), *prepared)
    cells = [list(range(i, i + targets)) for i in range(0, lanes * subs, targets)]
    arrived = lax.all_to_all(
        sent, ("mp", "sub"), 0, 0, axis_index_groups=cells, tiled=True
    )
    line_sum = arrived.astype(jnp.float32).sum(axis=0).astype(jnp.bfloat16)
    first_rows = part_rows * columns
    tiles = line_sum[:first_rows].reshape(docs, first_rows // docs, LANES)
    second = jnp.broadcast_to(line_sum[first_rows:][None], (docs, columns, LANES))
    arrived = lax.all_to_all(jnp.concatenate([tiles, second], axis=1), "docs", 0, 0, tiled=True)
    shard_sum = arrived.astype(jnp.float32).sum(axis=0)
    lambda_column, shard_sum = lax.optimization_barrier((lambda_column, shard_sum))
    own_grad = lax.dot_general(
        prepared[0][0], w_first, (((1,), (1,)), ((), ())), preferred_element_type=jnp.float32
    )
    emb_grad = (lambda_column * own_grad).astype(jnp.bfloat16)
    w_second_grad = shard_sum[first_rows // docs :].reshape(units)
    spread = sent_to_all(shard_sum[: first_rows // docs].astype(jnp.bfloat16), "docs")
    w_first_grad = (
        spread.reshape(columns, part_rows, LANES).transpose(1, 0, 2).reshape(part_rows, units)
    ).astype(jnp.float32)
    return (emb_grad, w_first_grad, w_second_grad)


def solution(mesh):
    split = ("groups", "docs", "mp", "sub")
    return jax.shard_map(
        on_device,
        mesh=mesh,
        in_specs=(P(split, None), P(split, None), P(split), P(split), P(), P()),
        out_specs=(P(split, None), P(("groups", "mp", "sub"), None), P("groups")),
        check_vma=False,
    )
```

```python
import functools

import jax
import jax.numpy as jnp
from jax import lax
from jax.experimental import pallas as pl
from jax.experimental.pallas import tpu as pltpu
from jax.sharding import PartitionSpec as P


LANES = 128


def whole(*shape_and_type):
    return jax.ShapeDtypeStruct(*shape_and_type)


def on_chip(x):
    return pltpu.with_memory_space_constraint(x, pltpu.VMEM)


def vmem_specs(count):
    return [pl.BlockSpec(memory_space=pltpu.VMEM)] * count


def score_kernel(capacity, emb_ref, w1_ref, w2_ref, owner_ref, query_ref, label_ref, sent_ref, slot_ref):
    rows = emb_ref.shape[0]
    halves = sent_ref.shape[1] // 4
    along = lax.broadcasted_iota(jnp.int32, (rows, rows), 1)
    down = lax.broadcasted_iota(jnp.int32, (rows, rows), 0)

    def column(row):
        return jnp.sum(jnp.where(along == down, row, 0), axis=1, keepdims=True)

    owner = owner_ref[...]
    owner_column = column(owner)
    earlier = jnp.where((owner_column == owner) & (along < down), 1, 0)
    slot = owner_column * capacity + jnp.sum(earlier, axis=1, keepdims=True)
    slot_ref[...] = slot
    mark = column(query_ref[...] + 1).astype(jnp.float32)
    label = column(label_ref[...]).astype(jnp.float32)

    pre_act = jnp.dot(emb_ref[...], w1_ref[...], preferred_element_type=jnp.float32)
    hidden = pre_act * jax.nn.sigmoid(pre_act)
    score = jnp.sum(hidden * w2_ref[...], axis=1, keepdims=True)

    lane = lax.broadcasted_iota(jnp.int32, (rows, LANES), 1)
    sent_ref[...] = jnp.zeros_like(sent_ref)
    for h in range(halves):
        here = slot == lane + h * LANES
        for place, value in enumerate((score, mark, label)):
            row = jnp.sum(jnp.where(here, value, 0.0), axis=0, keepdims=True)
            for target in range(sent_ref.shape[0]):
                sent_ref[target, place * halves + h : place * halves + h + 1, :] = row


def within_groups(x, capacity):
    lane = lax.broadcasted_iota(jnp.int32, x.shape, 1)
    out = [x]
    step = capacity // 2
    while step:
        upper = (lane & step) != 0
        spread = []
        for y in out:
            spread.append(jnp.where(upper, pltpu.roll(y, step, 1), y))
            spread.append(jnp.where(upper, y, pltpu.roll(y, LANES - step, 1)))
        out = spread
        step //= 2
    return out


def group_sum(x, capacity):
    lane = lax.broadcasted_iota(jnp.int32, x.shape, 1)
    step = capacity // 2
    while step:
        upper = (lane & step) != 0
        x = x + jnp.where(upper, pltpu.roll(x, step, 1), pltpu.roll(x, LANES - step, 1))
        step //= 2
    return x


def lambda_kernel(
    capacity, place_ref, got_ref, slot_ref, spread_ref, column_ref,
    score_by, mark_by, key_by, disc_by, row_scratch,
):
    sources = got_ref.shape[0]
    halves = got_ref.shape[1] // 4
    me = place_ref[0]
    rows = slot_ref.shape[0]
    source = lax.broadcasted_iota(jnp.int32, (sources, LANES), 0)
    lane = lax.broadcasted_iota(jnp.int32, (sources, LANES), 1)
    position = (source * capacity + lane % capacity).astype(jnp.float32)
    slots = float(sources * capacity)
    lane_of_row = lax.broadcasted_iota(jnp.int32, (rows, LANES), 1)
    lambda_column = jnp.zeros((rows, 1), jnp.float32)
    for h in range(halves):
        half_score = got_ref[:, h, :] * 0.5
        mark = got_ref[:, halves + h, :]
        label = got_ref[:, 2 * halves + h, :]
        key = label * slots - position
        for ref, value in ((score_by, half_score), (mark_by, mark), (key_by, key)):
            for c, spread in enumerate(within_groups(value, capacity)):
                ref[c * sources : (c + 1) * sources, :] = spread

        def rank_step(step, sums):
            soft, ideal = sums
            base = pl.multiple_of(step * 8, 8)
            score_rows = score_by[pl.ds(base, 8), :]
            mark_rows = mark_by[pl.ds(base, 8), :]
            key_rows = key_by[pl.ds(base, 8), :]
            for r in range(8):
                same = mark_rows[r : r + 1, :] == mark
                tilt = jnp.tanh(score_rows[r : r + 1, :] - half_score)
                soft = soft + jnp.where(same, tilt + 1.0, 0.0)
                ideal = ideal + jnp.where(same & (key_rows[r : r + 1, :] > key), 1.0, 0.0)
            return soft, ideal

        nothing = jnp.zeros((sources, LANES), jnp.float32)
        soft, ideal = lax.fori_loop(0, capacity * sources // 8, rank_step, (nothing, nothing))
        discount = 1.0 / jnp.log2(2.0 + (0.5 * soft - 0.5))
        gain = jnp.exp2(label) - 1.0
        term = gain / jnp.log2(2.0 + ideal)
        for c, spread in enumerate(within_groups(discount, capacity)):
            disc_by[c * sources : (c + 1) * sources, :] = spread

        for place, value in enumerate((half_score, mark, gain, discount)):
            row_scratch[place * sources : (place + 1) * sources, :] = value
        own_score, own_mark, own_gain, own_disc = (
            row_scratch[pl.ds(place * sources + me, 1), :] for place in range(4)
        )
        ideal_sum = jnp.zeros((1, LANES), jnp.float32)
        for query in range(2):
            asked = query + 1.0
            per_lane = jnp.sum(jnp.where(mark == asked, term, 0.0), axis=0, keepdims=True)
            spread = group_sum(jnp.broadcast_to(per_lane, (8, LANES)), capacity)[:1, :]
            ideal_sum = jnp.where(own_mark == asked, spread, ideal_sum)
        inv_ideal = jnp.where(ideal_sum > 0.0, 1.0 / jnp.where(ideal_sum > 0.0, ideal_sum, 1.0), 0.0)

        total = jnp.zeros((sources, LANES), jnp.float32)
        for c in range(capacity):
            at = slice(c * sources, (c + 1) * sources)
            their_gain = jnp.exp2(jnp.ceil(key_by[at, :] * (1.0 / slots))) - 1.0
            gain_gap = own_gain - their_gain
            gap = 2.0 * (score_by[at, :] - own_score)
            pull = jax.nn.sigmoid(jnp.where(gain_gap > 0.0, gap, -gap))
            pair = -gain_gap * jnp.abs(own_disc - disc_by[at, :]) * pull
            total = total + jnp.where(mark_by[at, :] == own_mark, pair, 0.0)
        lambda_row = jnp.sum(total, axis=0, keepdims=True) * inv_ideal
        here = slot_ref[...] == lane_of_row + h * LANES
        lambda_column = lambda_column + jnp.sum(
            jnp.where(here, lambda_row, 0.0), axis=1, keepdims=True
        )

    column_ref[...] = lambda_column
    along = lax.broadcasted_iota(jnp.int32, (rows, rows), 1)
    down = lax.broadcasted_iota(jnp.int32, (rows, rows), 0)
    row = jnp.sum(jnp.where(along == down, lambda_column, 0.0), axis=0, keepdims=True)
    spread_ref[...] = jnp.broadcast_to(row, spread_ref.shape)


def slope_kernel(count, place_ref, w1_ref, w2_ref, *refs):
    emb_refs, (slope_ref, hidden_ref, part_ref) = refs[:count], refs[count:]
    wide = part_ref.shape[2]
    mine = pl.ds(pl.multiple_of(place_ref[1] // 2 * wide, LANES), wide)
    for i, emb_ref in enumerate(emb_refs):
        pre_act = jnp.dot(emb_ref[...], w1_ref[...], preferred_element_type=jnp.float32)
        gate = jax.nn.sigmoid(pre_act)
        hidden_ref[i] = (pre_act * gate).astype(jnp.bfloat16)
        slope = gate * (1.0 + pre_act * (1.0 - gate))
        slope_ref[i] = (w2_ref[...] * slope).astype(jnp.bfloat16)
        part_ref[i] = emb_ref[:, mine]


def slopes(place, w_first, w2_row, blocks, wide):
    rows, units = blocks[0].shape[0], w_first.shape[1]
    count = len(blocks)
    return pl.pallas_call(
        functools.partial(slope_kernel, count),
        out_shape=(
            whole((count, rows, units), jnp.bfloat16),
            whole((count, rows, units), jnp.bfloat16),
            whole((count, rows, wide), jnp.bfloat16),
        ),
        in_specs=[pl.BlockSpec(memory_space=pltpu.SMEM)] + vmem_specs(2 + count),
        out_specs=tuple(vmem_specs(3)),
        name="slopes",
    )(place, w_first, w2_row, *blocks)


def product_kernel(*refs):
    lambda_refs, (slope_ref, hidden_ref, part_ref, sent_ref) = refs[:-4], refs[-4:]
    rows = part_ref.shape[1]
    along = lax.broadcasted_iota(jnp.int32, (rows, rows), 1)
    down = lax.broadcasted_iota(jnp.int32, (rows, rows), 0)
    total, second = None, None
    for i, lambda_ref in enumerate(lambda_refs):
        block = lambda_ref[...]
        column = jnp.sum(jnp.where(along == down, block[:1], 0.0), axis=1, keepdims=True)
        part = (part_ref[i].astype(jnp.float32) * column).astype(jnp.bfloat16)
        product = lax.dot_general(
            part, slope_ref[i], (((0,), (0,)), ((), ())), preferred_element_type=jnp.float32
        )
        high = block.astype(jnp.bfloat16)
        low = (block - high.astype(jnp.float32)).astype(jnp.bfloat16)
        hidden = hidden_ref[i]
        summed = jnp.dot(high, hidden, preferred_element_type=jnp.float32) + jnp.dot(
            low, hidden, preferred_element_type=jnp.float32
        )
        total = product if total is None else total + product
        second = summed if second is None else second + summed
    targets = sent_ref.shape[0]
    part_rows = total.shape[0] // targets
    columns = total.shape[1] // LANES
    rounded, second = total.astype(jnp.bfloat16), second.astype(jnp.bfloat16)
    for target in range(targets):
        for k in range(columns):
            at = slice(k * LANES, (k + 1) * LANES)
            sent_ref[target, k * part_rows : (k + 1) * part_rows, :] = rounded[
                target * part_rows : (target + 1) * part_rows, at
            ]
            row = part_rows * columns + k
            sent_ref[target, row : row + 1, :] = second[:1, at]


def sent_to_all(x, axis):
    count = lax.axis_size(axis)
    return lax.all_to_all(jnp.broadcast_to(x[None], (count, *x.shape)), axis, 0, 0, tiled=True)


def parity_blocks(block):
    lanes, subs = lax.axis_size("mp"), lax.axis_size("sub")

    def moved(x, by):
        return lax.ppermute(x, "mp", [(i, (i + by) % lanes) for i in range(lanes)])

    back, on = moved(block, 2), moved(block, -2)
    both_ways = [
        (i * subs + s, (i + (2 if s == 0 else -2)) % lanes * subs + s)
        for i in range(lanes)
        for s in range(subs)
    ]
    passed = jnp.where(lax.axis_index("sub") == 0, back, on)
    across = lax.ppermute(passed, ("mp", "sub"), both_ways)
    return back, on, across


def on_device(embeddings, owner_shard, query_local, labels, w_first, w_second):
    docs, lanes, subs = (lax.axis_size(axis) for axis in ("docs", "mp", "sub"))
    rows, width = embeddings.shape
    units = w_first.shape[1]
    capacity = 2 * rows // docs
    halves = docs * capacity // LANES
    w2_row = w_second.reshape(1, units)
    place = jnp.stack([lax.axis_index(axis) for axis in ("docs", "mp", "sub")]).astype(jnp.int32)
    back, on, across = parity_blocks(embeddings)
    sent, slot = pl.pallas_call(
        functools.partial(score_kernel, capacity),
        out_shape=(
            whole((docs, 4 * halves, LANES), jnp.float32),
            whole((rows, 1), jnp.int32),
        ),
        in_specs=vmem_specs(6),
        out_specs=tuple(vmem_specs(2)),
        name="score",
    )(
        embeddings, w_first, w2_row,
        owner_shard.reshape(1, rows), query_local.reshape(1, rows), labels.reshape(1, rows),
    )
    got = lax.all_to_all(sent, "docs", 0, 0, tiled=True)
    spread, lambda_column = pl.pallas_call(
        functools.partial(lambda_kernel, capacity),
        out_shape=(whole((8, rows), jnp.float32), whole((rows, 1), jnp.float32)),
        in_specs=[pl.BlockSpec(memory_space=pltpu.SMEM)] + vmem_specs(2),
        out_specs=tuple(vmem_specs(2)),
        scratch_shapes=[pltpu.VMEM((docs * capacity, LANES), jnp.float32)] * 4
        + [pltpu.VMEM((4 * docs, LANES), jnp.float32)],
        name="lambdas",
    )(place, on_chip(got), slot)
    gathered = [
        lax.ppermute(spread, "mp", [(i, (i + by) % lanes) for i in range(lanes)])
        for by in (lanes // 2, 2, -2)
    ]
    across_lambdas, back_lambdas, on_lambdas = (on_chip(x) for x in gathered)

    part_rows = width // (lanes * subs)
    targets = 2 * subs
    wide = targets * part_rows
    columns = units // LANES
    prepared = slopes(place, w_first, w2_row, [embeddings, back, on, across], wide)
    sent = pl.pallas_call(
        product_kernel,
        out_shape=pltpu.VMEM((targets, (part_rows + 1) * columns, LANES), jnp.bfloat16),
        in_specs=vmem_specs(7),
        out_specs=vmem_specs(1)[0],
        name="product",
    )(spread, back_lambdas, on_lambdas, across_lambdas, *prepared)
    cells = [list(range(i, i + targets)) for i in range(0, lanes * subs, targets)]
    arrived = lax.all_to_all(
        sent, ("mp", "sub"), 0, 0, axis_index_groups=cells, tiled=True
    )
    line_sum = arrived.astype(jnp.float32).sum(axis=0).astype(jnp.bfloat16)
    first_rows = part_rows * columns
    tiles = line_sum[:first_rows].reshape(docs, first_rows // docs, LANES)
    second = jnp.broadcast_to(line_sum[first_rows:][None], (docs, columns, LANES))
    arrived = lax.all_to_all(jnp.concatenate([tiles, second], axis=1), "docs", 0, 0, tiled=True)
    shard_sum = arrived.astype(jnp.float32).sum(axis=0)
    lambda_column, shard_sum = lax.optimization_barrier((lambda_column, shard_sum))
    own_grad = lax.dot_general(
        prepared[0][0], w_first, (((1,), (1,)), ((), ())), preferred_element_type=jnp.float32
    )
    emb_grad = (lambda_column * own_grad).astype(jnp.bfloat16)
    w_second_grad = shard_sum[first_rows // docs :].reshape(units)
    spread = sent_to_all(shard_sum[: first_rows // docs].astype(jnp.bfloat16), "docs")
    w_first_grad = (
        spread.reshape(columns, part_rows, LANES).transpose(1, 0, 2).reshape(part_rows, units)
    ).astype(jnp.float32)
    return (emb_grad, w_first_grad, w_second_grad)


def solution(mesh):
    split = ("groups", "docs", "mp", "sub")
    return jax.shard_map(
        on_device,
        mesh=mesh,
        in_specs=(P(split, None), P(split, None), P(split), P(split), P(), P()),
        out_specs=(P(split, None), P(("groups", "mp", "sub"), None), P("groups")),
        check_vma=False,
    )
```

```python
import functools

import jax
import jax.numpy as jnp
from jax import lax
from jax.experimental import pallas as pl
from jax.experimental.pallas import tpu as pltpu
from jax.sharding import PartitionSpec as P


LANES = 128


def whole(*shape_and_type):
    return jax.ShapeDtypeStruct(*shape_and_type)


def on_chip(x):
    return pltpu.with_memory_space_constraint(x, pltpu.VMEM)


def vmem_specs(count):
    return [pl.BlockSpec(memory_space=pltpu.VMEM)] * count


def score_kernel(capacity, emb_ref, w1_ref, w2_ref, owner_ref, query_ref, label_ref, sent_ref, slot_ref):
    rows = emb_ref.shape[0]
    halves = sent_ref.shape[1] // 4
    along = lax.broadcasted_iota(jnp.int32, (rows, rows), 1)
    down = lax.broadcasted_iota(jnp.int32, (rows, rows), 0)

    def column(row):
        return jnp.sum(jnp.where(along == down, row, 0), axis=1, keepdims=True)

    owner = owner_ref[...]
    owner_column = column(owner)
    earlier = jnp.where((owner_column == owner) & (along < down), 1, 0)
    slot = owner_column * capacity + jnp.sum(earlier, axis=1, keepdims=True)
    slot_ref[...] = slot
    mark = column(query_ref[...] + 1).astype(jnp.float32)
    label = column(label_ref[...]).astype(jnp.float32)

    pre_act = jnp.dot(emb_ref[...], w1_ref[...], preferred_element_type=jnp.float32)
    hidden = pre_act * jax.nn.sigmoid(pre_act)
    score = jnp.sum(hidden * w2_ref[...], axis=1, keepdims=True)

    lane = lax.broadcasted_iota(jnp.int32, (rows, LANES), 1)
    sent_ref[...] = jnp.zeros_like(sent_ref)
    for h in range(halves):
        here = slot == lane + h * LANES
        for place, value in enumerate((score, mark, label)):
            row = jnp.sum(jnp.where(here, value, 0.0), axis=0, keepdims=True)
            for target in range(sent_ref.shape[0]):
                sent_ref[target, place * halves + h : place * halves + h + 1, :] = row


def within_groups(x, capacity):
    lane = lax.broadcasted_iota(jnp.int32, x.shape, 1)
    out = [x]
    step = capacity // 2
    while step:
        upper = (lane & step) != 0
        spread = []
        for y in out:
            spread.append(jnp.where(upper, pltpu.roll(y, step, 1), y))
            spread.append(jnp.where(upper, y, pltpu.roll(y, LANES - step, 1)))
        out = spread
        step //= 2
    return out


def group_sum(x, capacity):
    lane = lax.broadcasted_iota(jnp.int32, x.shape, 1)
    step = capacity // 2
    while step:
        upper = (lane & step) != 0
        x = x + jnp.where(upper, pltpu.roll(x, step, 1), pltpu.roll(x, LANES - step, 1))
        step //= 2
    return x


def lambda_kernel(
    capacity, place_ref, got_ref, slot_ref, spread_ref, column_ref,
    score_by, mark_by, key_by, disc_by, row_scratch,
):
    sources = got_ref.shape[0]
    halves = got_ref.shape[1] // 4
    me = place_ref[0]
    rows = slot_ref.shape[0]
    source = lax.broadcasted_iota(jnp.int32, (sources, LANES), 0)
    lane = lax.broadcasted_iota(jnp.int32, (sources, LANES), 1)
    position = (source * capacity + lane % capacity).astype(jnp.float32)
    slots = float(sources * capacity)
    lane_of_row = lax.broadcasted_iota(jnp.int32, (rows, LANES), 1)
    lambda_column = jnp.zeros((rows, 1), jnp.float32)
    for h in range(halves):
        half_score = got_ref[:, h, :] * 0.5
        mark = got_ref[:, halves + h, :]
        label = got_ref[:, 2 * halves + h, :]
        key = label * slots - position
        for ref, value in ((score_by, half_score), (mark_by, mark), (key_by, key)):
            for c, spread in enumerate(within_groups(value, capacity)):
                ref[c * sources : (c + 1) * sources, :] = spread

        def rank_step(step, sums):
            soft, ideal = sums
            base = pl.multiple_of(step * 8, 8)
            score_rows = score_by[pl.ds(base, 8), :]
            mark_rows = mark_by[pl.ds(base, 8), :]
            key_rows = key_by[pl.ds(base, 8), :]
            for r in range(8):
                same = mark_rows[r : r + 1, :] == mark
                tilt = jnp.tanh(score_rows[r : r + 1, :] - half_score)
                soft = soft + jnp.where(same, tilt + 1.0, 0.0)
                ideal = ideal + jnp.where(same & (key_rows[r : r + 1, :] > key), 1.0, 0.0)
            return soft, ideal

        nothing = jnp.zeros((sources, LANES), jnp.float32)
        soft, ideal = lax.fori_loop(0, capacity * sources // 8, rank_step, (nothing, nothing))
        discount = 1.0 / jnp.log2(2.0 + (0.5 * soft - 0.5))
        gain = jnp.exp2(label) - 1.0
        term = gain / jnp.log2(2.0 + ideal)
        for c, spread in enumerate(within_groups(discount, capacity)):
            disc_by[c * sources : (c + 1) * sources, :] = spread

        for place, value in enumerate((half_score, mark, gain, discount)):
            row_scratch[place * sources : (place + 1) * sources, :] = value
        own_score, own_mark, own_gain, own_disc = (
            row_scratch[pl.ds(place * sources + me, 1), :] for place in range(4)
        )
        ideal_sum = jnp.zeros((1, LANES), jnp.float32)
        for query in range(2):
            asked = query + 1.0
            per_lane = jnp.sum(jnp.where(mark == asked, term, 0.0), axis=0, keepdims=True)
            spread = group_sum(jnp.broadcast_to(per_lane, (8, LANES)), capacity)[:1, :]
            ideal_sum = jnp.where(own_mark == asked, spread, ideal_sum)
        inv_ideal = jnp.where(ideal_sum > 0.0, 1.0 / jnp.where(ideal_sum > 0.0, ideal_sum, 1.0), 0.0)

        total = jnp.zeros((sources, LANES), jnp.float32)
        for c in range(capacity):
            at = slice(c * sources, (c + 1) * sources)
            their_gain = jnp.exp2(jnp.ceil(key_by[at, :] * (1.0 / slots))) - 1.0
            gain_gap = own_gain - their_gain
            gap = 2.0 * (score_by[at, :] - own_score)
            pull = jax.nn.sigmoid(jnp.where(gain_gap > 0.0, gap, -gap))
            pair = -gain_gap * jnp.abs(own_disc - disc_by[at, :]) * pull
            total = total + jnp.where(mark_by[at, :] == own_mark, pair, 0.0)
        lambda_row = jnp.sum(total, axis=0, keepdims=True) * inv_ideal
        here = slot_ref[...] == lane_of_row + h * LANES
        lambda_column = lambda_column + jnp.sum(
            jnp.where(here, lambda_row, 0.0), axis=1, keepdims=True
        )

    column_ref[...] = lambda_column
    along = lax.broadcasted_iota(jnp.int32, (rows, rows), 1)
    down = lax.broadcasted_iota(jnp.int32, (rows, rows), 0)
    row = jnp.sum(jnp.where(along == down, lambda_column, 0.0), axis=0, keepdims=True)
    spread_ref[...] = jnp.broadcast_to(row[None], spread_ref.shape)


def slope_kernel(count, place_ref, w1_ref, w2_ref, *refs):
    emb_refs, (slope_ref, hidden_ref, part_ref) = refs[:count], refs[count:]
    wide = part_ref.shape[2]
    mine = pl.ds(pl.multiple_of(place_ref[1] // 2 * wide, LANES), wide)
    for i, emb_ref in enumerate(emb_refs):
        pre_act = jnp.dot(emb_ref[...], w1_ref[...], preferred_element_type=jnp.float32)
        gate = jax.nn.sigmoid(pre_act)
        hidden_ref[i] = (pre_act * gate).astype(jnp.bfloat16)
        slope = gate * (1.0 + pre_act * (1.0 - gate))
        slope_ref[i] = (w2_ref[...] * slope).astype(jnp.bfloat16)
        part_ref[i] = emb_ref[:, mine]


def slopes(place, w_first, w2_row, blocks, wide):
    rows, units = blocks[0].shape[0], w_first.shape[1]
    count = len(blocks)
    return pl.pallas_call(
        functools.partial(slope_kernel, count),
        out_shape=(
            whole((count, rows, units), jnp.bfloat16),
            whole((count, rows, units), jnp.bfloat16),
            whole((count, rows, wide), jnp.bfloat16),
        ),
        in_specs=[pl.BlockSpec(memory_space=pltpu.SMEM)] + vmem_specs(2 + count),
        out_specs=tuple(vmem_specs(3)),
        name="slopes",
    )(place, w_first, w2_row, *blocks)


def product_kernel(groups, place_ref, lambda_ref, *refs):
    inputs, sent_ref = refs[: 3 * len(groups)], refs[-1]
    members, rows = lambda_ref.shape[0], lambda_ref.shape[2]
    my_member = place_ref[1] // 2
    along = lax.broadcasted_iota(jnp.int32, (rows, rows), 1)
    down = lax.broadcasted_iota(jnp.int32, (rows, rows), 0)
    total, second = None, None
    for g, offsets in enumerate(groups):
        slope_ref, hidden_ref, part_ref = inputs[3 * g : 3 * g + 3]
        for i, offset in enumerate(offsets):
            block = lambda_ref[lax.rem(my_member + offset, members)]
            column = jnp.sum(jnp.where(along == down, block[:1], 0.0), axis=1, keepdims=True)
            part = (part_ref[i].astype(jnp.float32) * column).astype(jnp.bfloat16)
            product = lax.dot_general(
                part, slope_ref[i], (((0,), (0,)), ((), ())), preferred_element_type=jnp.float32
            )
            high = block.astype(jnp.bfloat16)
            low = (block - high.astype(jnp.float32)).astype(jnp.bfloat16)
            hidden = hidden_ref[i]
            summed = jnp.dot(high, hidden, preferred_element_type=jnp.float32) + jnp.dot(
                low, hidden, preferred_element_type=jnp.float32
            )
            total = product if total is None else total + product
            second = summed if second is None else second + summed
    targets = sent_ref.shape[0]
    part_rows = total.shape[0] // targets
    columns = total.shape[1] // LANES
    rounded, second = total.astype(jnp.bfloat16), second.astype(jnp.bfloat16)
    for target in range(targets):
        for k in range(columns):
            at = slice(k * LANES, (k + 1) * LANES)
            sent_ref[target, k * part_rows : (k + 1) * part_rows, :] = rounded[
                target * part_rows : (target + 1) * part_rows, at
            ]
            row = part_rows * columns + k
            sent_ref[target, row : row + 1, :] = second[:1, at]


def sent_to_all(x, axis):
    count = lax.axis_size(axis)
    return lax.all_to_all(jnp.broadcast_to(x[None], (count, *x.shape)), axis, 0, 0, tiled=True)


def parity_blocks(block):
    lanes, subs = lax.axis_size("mp"), lax.axis_size("sub")

    def moved(x, by):
        return lax.ppermute(x, "mp", [(i, (i + by) % lanes) for i in range(lanes)])

    back, on = moved(block, 2), moved(block, -2)
    both_ways = [
        (i * subs + s, (i + (2 if s == 0 else -2)) % lanes * subs + s)
        for i in range(lanes)
        for s in range(subs)
    ]
    passed = jnp.where(lax.axis_index("sub") == 0, back, on)
    across = lax.ppermute(passed, ("mp", "sub"), both_ways)
    return back, on, across


def on_device(embeddings, owner_shard, query_local, labels, w_first, w_second):
    docs, lanes, subs = (lax.axis_size(axis) for axis in ("docs", "mp", "sub"))
    rows, width = embeddings.shape
    units = w_first.shape[1]
    capacity = 2 * rows // docs
    halves = docs * capacity // LANES
    w2_row = w_second.reshape(1, units)
    place = jnp.stack([lax.axis_index(axis) for axis in ("docs", "mp", "sub")]).astype(jnp.int32)
    back, on, across = parity_blocks(embeddings)
    members = lanes // 2
    sent, slot = pl.pallas_call(
        functools.partial(score_kernel, capacity),
        out_shape=(
            whole((docs, 4 * halves, LANES), jnp.float32),
            whole((rows, 1), jnp.int32),
        ),
        in_specs=vmem_specs(6),
        out_specs=tuple(vmem_specs(2)),
        name="score",
    )(
        embeddings, w_first, w2_row,
        owner_shard.reshape(1, rows), query_local.reshape(1, rows), labels.reshape(1, rows),
    )
    got = lax.all_to_all(sent, "docs", 0, 0, tiled=True)
    spread, lambda_column = pl.pallas_call(
        functools.partial(lambda_kernel, capacity),
        out_shape=(whole((members, 8, rows), jnp.float32), whole((rows, 1), jnp.float32)),
        in_specs=[pl.BlockSpec(memory_space=pltpu.SMEM)] + vmem_specs(2),
        out_specs=tuple(vmem_specs(2)),
        scratch_shapes=[pltpu.VMEM((docs * capacity, LANES), jnp.float32)] * 4
        + [pltpu.VMEM((4 * docs, LANES), jnp.float32)],
        name="lambdas",
    )(place, on_chip(got), slot)
    parities = [list(range(parity, lanes, 2)) for parity in range(2)]
    all_lambdas = lax.all_to_all(
        spread, "mp", 0, 0, axis_index_groups=parities, tiled=True
    )

    part_rows = width // (lanes * subs)
    targets = 2 * subs
    wide = targets * part_rows
    columns = units // LANES
    prepared = slopes(place, w_first, w2_row, [embeddings, back, on, across], wide)
    offsets = ((0, members - 1, 1, 2),)
    sent = pl.pallas_call(
        functools.partial(product_kernel, offsets),
        out_shape=pltpu.VMEM((targets, (part_rows + 1) * columns, LANES), jnp.bfloat16),
        in_specs=[pl.BlockSpec(memory_space=pltpu.SMEM)] + vmem_specs(4),
        out_specs=vmem_specs(1)[0],
        name="product",
    )(place, on_chip(all_lambdas), *prepared)
    cells = [list(range(i, i + targets)) for i in range(0, lanes * subs, targets)]
    arrived = lax.all_to_all(
        sent, ("mp", "sub"), 0, 0, axis_index_groups=cells, tiled=True
    )
    line_sum = arrived.astype(jnp.float32).sum(axis=0).astype(jnp.bfloat16)
    first_rows = part_rows * columns
    tiles = line_sum[:first_rows].reshape(docs, first_rows // docs, LANES)
    second = jnp.broadcast_to(line_sum[first_rows:][None], (docs, columns, LANES))
    arrived = lax.all_to_all(jnp.concatenate([tiles, second], axis=1), "docs", 0, 0, tiled=True)
    shard_sum = arrived.astype(jnp.float32).sum(axis=0)
    lambda_column, shard_sum = lax.optimization_barrier((lambda_column, shard_sum))
    own_grad = lax.dot_general(
        prepared[0][0], w_first, (((1,), (1,)), ((), ())), preferred_element_type=jnp.float32
    )
    emb_grad = (lambda_column * own_grad).astype(jnp.bfloat16)
    w_second_grad = shard_sum[first_rows // docs :].reshape(units)
    spread = sent_to_all(shard_sum[: first_rows // docs].astype(jnp.bfloat16), "docs")
    w_first_grad = (
        spread.reshape(columns, part_rows, LANES).transpose(1, 0, 2).reshape(part_rows, units)
    ).astype(jnp.float32)
    return (emb_grad, w_first_grad, w_second_grad)


def solution(mesh):
    split = ("groups", "docs", "mp", "sub")
    return jax.shard_map(
        on_device,
        mesh=mesh,
        in_specs=(P(split, None), P(split, None), P(split), P(split), P(), P()),
        out_specs=(P(split, None), P(("groups", "mp", "sub"), None), P("groups")),
        check_vma=False,
    )
```

```python
import functools

import jax
import jax.numpy as jnp
from jax import lax
from jax.experimental import pallas as pl
from jax.experimental.pallas import tpu as pltpu
from jax.sharding import PartitionSpec as P


LANES = 128


def whole(*shape_and_type):
    return jax.ShapeDtypeStruct(*shape_and_type)


def on_chip(x):
    return pltpu.with_memory_space_constraint(x, pltpu.VMEM)


def vmem_specs(count):
    return [pl.BlockSpec(memory_space=pltpu.VMEM)] * count


def score_kernel(capacity, emb_ref, w1_ref, w2_ref, owner_ref, query_ref, label_ref, sent_ref, slot_ref):
    rows = emb_ref.shape[0]
    halves = sent_ref.shape[1] // 4
    along = lax.broadcasted_iota(jnp.int32, (rows, rows), 1)
    down = lax.broadcasted_iota(jnp.int32, (rows, rows), 0)

    def column(row):
        return jnp.sum(jnp.where(along == down, row, 0), axis=1, keepdims=True)

    owner = owner_ref[...]
    owner_column = column(owner)
    earlier = jnp.where((owner_column == owner) & (along < down), 1, 0)
    slot = owner_column * capacity + jnp.sum(earlier, axis=1, keepdims=True)
    slot_ref[...] = slot
    mark = column(query_ref[...] + 1).astype(jnp.float32)
    label = column(label_ref[...]).astype(jnp.float32)

    pre_act = jnp.dot(emb_ref[...], w1_ref[...], preferred_element_type=jnp.float32)
    hidden = pre_act * jax.nn.sigmoid(pre_act)
    score = jnp.sum(hidden * w2_ref[...], axis=1, keepdims=True)

    lane = lax.broadcasted_iota(jnp.int32, (rows, LANES), 1)
    sent_ref[...] = jnp.zeros_like(sent_ref)
    for h in range(halves):
        here = slot == lane + h * LANES
        for place, value in enumerate((score, mark, label)):
            row = jnp.sum(jnp.where(here, value, 0.0), axis=0, keepdims=True)
            for target in range(sent_ref.shape[0]):
                sent_ref[target, place * halves + h : place * halves + h + 1, :] = row


def within_groups(x, capacity):
    lane = lax.broadcasted_iota(jnp.int32, x.shape, 1)
    out = [x]
    step = capacity // 2
    while step:
        upper = (lane & step) != 0
        spread = []
        for y in out:
            spread.append(jnp.where(upper, pltpu.roll(y, step, 1), y))
            spread.append(jnp.where(upper, y, pltpu.roll(y, LANES - step, 1)))
        out = spread
        step //= 2
    return out


def group_sum(x, capacity):
    lane = lax.broadcasted_iota(jnp.int32, x.shape, 1)
    step = capacity // 2
    while step:
        upper = (lane & step) != 0
        x = x + jnp.where(upper, pltpu.roll(x, step, 1), pltpu.roll(x, LANES - step, 1))
        step //= 2
    return x


def lambda_kernel(
    capacity, place_ref, got_ref, slot_ref, spread_ref, column_ref,
    score_by, mark_by, key_by, disc_by, row_scratch,
):
    sources = got_ref.shape[0]
    halves = got_ref.shape[1] // 4
    me = place_ref[0]
    rows = slot_ref.shape[0]
    source = lax.broadcasted_iota(jnp.int32, (sources, LANES), 0)
    lane = lax.broadcasted_iota(jnp.int32, (sources, LANES), 1)
    position = (source * capacity + lane % capacity).astype(jnp.float32)
    slots = float(sources * capacity)
    trip = 2 * sources
    lane_of_row = lax.broadcasted_iota(jnp.int32, (rows, LANES), 1)
    lambda_column = jnp.zeros((rows, 1), jnp.float32)
    for h in range(halves):
        half_score = got_ref[:, h, :] * 0.5
        mark = got_ref[:, halves + h, :]
        label = got_ref[:, 2 * halves + h, :]
        key = (label + 8.0 * mark) * slots - position
        counts = []
        for query in range(2):
            here = jnp.sum(jnp.where(mark == query + 1.0, 1.0, 0.0), axis=0, keepdims=True)
            counts.append(group_sum(jnp.broadcast_to(here, (8, LANES)), capacity)[:1, :])
        first, other = counts
        fellows = jnp.where(mark == 1.0, first, jnp.where(mark == 2.0, other, slots - first - other))
        above = jnp.where(mark == 1.0, other, jnp.where(mark == 2.0, 0.0, first + other))
        for ref, value in ((score_by, half_score), (mark_by, mark), (key_by, key)):
            for c, spread in enumerate(within_groups(value, capacity)):
                ref[c * sources : (c + 1) * sources, :] = spread

        def rank_step(step, sums):
            soft, ideal = sums
            base = pl.multiple_of(step * trip, trip)
            score_rows = score_by[pl.ds(base, trip), :]
            mark_rows = mark_by[pl.ds(base, trip), :]
            key_rows = key_by[pl.ds(base, trip), :]
            for r in range(trip):
                same = mark_rows[r : r + 1, :] == mark
                tilt = jnp.tanh(score_rows[r : r + 1, :] - half_score)
                soft = soft + jnp.where(same, tilt, 0.0)
                ideal = ideal + jnp.where(key_rows[r : r + 1, :] > key, 1.0, 0.0)
            return soft, ideal

        nothing = jnp.zeros((sources, LANES), jnp.float32)
        soft, ideal = lax.fori_loop(0, capacity * sources // trip, rank_step, (nothing, nothing))
        discount = 1.0 / jnp.log2(2.0 + (0.5 * (soft + fellows) - 0.5))
        gain = jnp.exp2(label) - 1.0
        term = gain / jnp.log2(2.0 + (ideal - above))
        for c, spread in enumerate(within_groups(discount, capacity)):
            disc_by[c * sources : (c + 1) * sources, :] = spread

        for place, value in enumerate((half_score, mark, gain, discount)):
            row_scratch[place * sources : (place + 1) * sources, :] = value
        own_score, own_mark, own_gain, own_disc = (
            row_scratch[pl.ds(place * sources + me, 1), :] for place in range(4)
        )
        ideal_sum = jnp.zeros((1, LANES), jnp.float32)
        for query in range(2):
            asked = query + 1.0
            per_lane = jnp.sum(jnp.where(mark == asked, term, 0.0), axis=0, keepdims=True)
            spread = group_sum(jnp.broadcast_to(per_lane, (8, LANES)), capacity)[:1, :]
            ideal_sum = jnp.where(own_mark == asked, spread, ideal_sum)
        inv_ideal = jnp.where(ideal_sum > 0.0, 1.0 / jnp.where(ideal_sum > 0.0, ideal_sum, 1.0), 0.0)

        total = jnp.zeros((sources, LANES), jnp.float32)
        for c in range(capacity):
            at = slice(c * sources, (c + 1) * sources)
            their_label = jnp.ceil(key_by[at, :] * (1.0 / slots)) - 8.0 * mark_by[at, :]
            their_gain = jnp.exp2(their_label) - 1.0
            gain_gap = own_gain - their_gain
            gap = 2.0 * (score_by[at, :] - own_score)
            pull = jax.nn.sigmoid(jnp.where(gain_gap > 0.0, gap, -gap))
            pair = -gain_gap * jnp.abs(own_disc - disc_by[at, :]) * pull
            total = total + jnp.where(mark_by[at, :] == own_mark, pair, 0.0)
        lambda_row = jnp.sum(total, axis=0, keepdims=True) * inv_ideal
        here = slot_ref[...] == lane_of_row + h * LANES
        lambda_column = lambda_column + jnp.sum(
            jnp.where(here, lambda_row, 0.0), axis=1, keepdims=True
        )

    column_ref[...] = lambda_column
    along = lax.broadcasted_iota(jnp.int32, (rows, rows), 1)
    down = lax.broadcasted_iota(jnp.int32, (rows, rows), 0)
    row = jnp.sum(jnp.where(along == down, lambda_column, 0.0), axis=0, keepdims=True)
    spread_ref[...] = jnp.broadcast_to(row[None], spread_ref.shape)


def slope_kernel(count, place_ref, w1_ref, w2_ref, *refs):
    emb_refs, (slope_ref, hidden_ref, part_ref) = refs[:count], refs[count:]
    wide = part_ref.shape[2]
    mine = pl.ds(pl.multiple_of(place_ref[1] // 2 * wide, LANES), wide)
    for i, emb_ref in enumerate(emb_refs):
        pre_act = jnp.dot(emb_ref[...], w1_ref[...], preferred_element_type=jnp.float32)
        gate = jax.nn.sigmoid(pre_act)
        hidden_ref[i] = (pre_act * gate).astype(jnp.bfloat16)
        slope = gate * (1.0 + pre_act * (1.0 - gate))
        slope_ref[i] = (w2_ref[...] * slope).astype(jnp.bfloat16)
        part_ref[i] = emb_ref[:, mine]


def slopes(place, w_first, w2_row, blocks, wide):
    rows, units = blocks[0].shape[0], w_first.shape[1]
    count = len(blocks)
    return pl.pallas_call(
        functools.partial(slope_kernel, count),
        out_shape=(
            whole((count, rows, units), jnp.bfloat16),
            whole((count, rows, units), jnp.bfloat16),
            whole((count, rows, wide), jnp.bfloat16),
        ),
        in_specs=[pl.BlockSpec(memory_space=pltpu.SMEM)] + vmem_specs(2 + count),
        out_specs=tuple(vmem_specs(3)),
        name="slopes",
    )(place, w_first, w2_row, *blocks)


def product_kernel(groups, place_ref, lambda_ref, *refs):
    inputs, sent_ref = refs[: 3 * len(groups)], refs[-1]
    members, rows = lambda_ref.shape[0], lambda_ref.shape[2]
    my_member = place_ref[1] // 2
    along = lax.broadcasted_iota(jnp.int32, (rows, rows), 1)
    down = lax.broadcasted_iota(jnp.int32, (rows, rows), 0)
    total, second = None, None
    for g, offsets in enumerate(groups):
        slope_ref, hidden_ref, part_ref = inputs[3 * g : 3 * g + 3]
        for i, offset in enumerate(offsets):
            block = lambda_ref[lax.rem(my_member + offset, members)]
            column = jnp.sum(jnp.where(along == down, block[:1], 0.0), axis=1, keepdims=True)
            part = (part_ref[i].astype(jnp.float32) * column).astype(jnp.bfloat16)
            product = lax.dot_general(
                part, slope_ref[i], (((0,), (0,)), ((), ())), preferred_element_type=jnp.float32
            )
            high = block.astype(jnp.bfloat16)
            low = (block - high.astype(jnp.float32)).astype(jnp.bfloat16)
            hidden = hidden_ref[i]
            summed = jnp.dot(high, hidden, preferred_element_type=jnp.float32) + jnp.dot(
                low, hidden, preferred_element_type=jnp.float32
            )
            total = product if total is None else total + product
            second = summed if second is None else second + summed
    targets = sent_ref.shape[0]
    part_rows = total.shape[0] // targets
    columns = total.shape[1] // LANES
    rounded, second = total.astype(jnp.bfloat16), second.astype(jnp.bfloat16)
    for target in range(targets):
        for k in range(columns):
            at = slice(k * LANES, (k + 1) * LANES)
            sent_ref[target, k * part_rows : (k + 1) * part_rows, :] = rounded[
                target * part_rows : (target + 1) * part_rows, at
            ]
            row = part_rows * columns + k
            sent_ref[target, row : row + 1, :] = second[:1, at]


def sent_to_all(x, axis):
    count = lax.axis_size(axis)
    return lax.all_to_all(jnp.broadcast_to(x[None], (count, *x.shape)), axis, 0, 0, tiled=True)


def parity_blocks(block):
    lanes, subs = lax.axis_size("mp"), lax.axis_size("sub")

    def moved(x, by):
        return lax.ppermute(x, "mp", [(i, (i + by) % lanes) for i in range(lanes)])

    back, on = moved(block, 2), moved(block, -2)
    both_ways = [
        (i * subs + s, (i + (2 if s == 0 else -2)) % lanes * subs + s)
        for i in range(lanes)
        for s in range(subs)
    ]
    passed = jnp.where(lax.axis_index("sub") == 0, back, on)
    across = lax.ppermute(passed, ("mp", "sub"), both_ways)
    return back, on, across


def on_device(embeddings, owner_shard, query_local, labels, w_first, w_second):
    docs, lanes, subs = (lax.axis_size(axis) for axis in ("docs", "mp", "sub"))
    rows, width = embeddings.shape
    units = w_first.shape[1]
    capacity = 2 * rows // docs
    halves = docs * capacity // LANES
    w2_row = w_second.reshape(1, units)
    place = jnp.stack([lax.axis_index(axis) for axis in ("docs", "mp", "sub")]).astype(jnp.int32)
    back, on, across = parity_blocks(embeddings)
    members = lanes // 2
    sent, slot = pl.pallas_call(
        functools.partial(score_kernel, capacity),
        out_shape=(
            whole((docs, 4 * halves, LANES), jnp.float32),
            whole((rows, 1), jnp.int32),
        ),
        in_specs=vmem_specs(6),
        out_specs=tuple(vmem_specs(2)),
        name="score",
    )(
        embeddings, w_first, w2_row,
        owner_shard.reshape(1, rows), query_local.reshape(1, rows), labels.reshape(1, rows),
    )
    got = lax.all_to_all(sent, "docs", 0, 0, tiled=True)
    spread, lambda_column = pl.pallas_call(
        functools.partial(lambda_kernel, capacity),
        out_shape=(whole((members, 8, rows), jnp.float32), whole((rows, 1), jnp.float32)),
        in_specs=[pl.BlockSpec(memory_space=pltpu.SMEM)] + vmem_specs(2),
        out_specs=tuple(vmem_specs(2)),
        scratch_shapes=[pltpu.VMEM((docs * capacity, LANES), jnp.float32)] * 4
        + [pltpu.VMEM((4 * docs, LANES), jnp.float32)],
        name="lambdas",
    )(place, on_chip(got), slot)
    parities = [list(range(parity, lanes, 2)) for parity in range(2)]
    all_lambdas = lax.all_to_all(
        spread, "mp", 0, 0, axis_index_groups=parities, tiled=True
    )

    part_rows = width // (lanes * subs)
    targets = 2 * subs
    wide = targets * part_rows
    columns = units // LANES
    prepared = slopes(place, w_first, w2_row, [embeddings, back, on, across], wide)
    offsets = ((0, members - 1, 1, 2),)
    sent = pl.pallas_call(
        functools.partial(product_kernel, offsets),
        out_shape=pltpu.VMEM((targets, (part_rows + 1) * columns, LANES), jnp.bfloat16),
        in_specs=[pl.BlockSpec(memory_space=pltpu.SMEM)] + vmem_specs(4),
        out_specs=vmem_specs(1)[0],
        name="product",
    )(place, on_chip(all_lambdas), *prepared)
    cells = [list(range(i, i + targets)) for i in range(0, lanes * subs, targets)]
    arrived = lax.all_to_all(
        sent, ("mp", "sub"), 0, 0, axis_index_groups=cells, tiled=True
    )
    line_sum = arrived.astype(jnp.float32).sum(axis=0).astype(jnp.bfloat16)
    first_rows = part_rows * columns
    tiles = line_sum[:first_rows].reshape(docs, first_rows // docs, LANES)
    second = jnp.broadcast_to(line_sum[first_rows:][None], (docs, columns, LANES))
    arrived = lax.all_to_all(jnp.concatenate([tiles, second], axis=1), "docs", 0, 0, tiled=True)
    shard_sum = arrived.astype(jnp.float32).sum(axis=0)
    lambda_column, shard_sum = lax.optimization_barrier((lambda_column, shard_sum))
    own_grad = lax.dot_general(
        prepared[0][0], w_first, (((1,), (1,)), ((), ())), preferred_element_type=jnp.float32
    )
    emb_grad = (lambda_column * own_grad).astype(jnp.bfloat16)
    w_second_grad = shard_sum[first_rows // docs :].reshape(units)
    spread = sent_to_all(shard_sum[: first_rows // docs].astype(jnp.bfloat16), "docs")
    w_first_grad = (
        spread.reshape(columns, part_rows, LANES).transpose(1, 0, 2).reshape(part_rows, units)
    ).astype(jnp.float32)
    return (emb_grad, w_first_grad, w_second_grad)


def solution(mesh):
    split = ("groups", "docs", "mp", "sub")
    return jax.shard_map(
        on_device,
        mesh=mesh,
        in_specs=(P(split, None), P(split, None), P(split), P(split), P(), P()),
        out_specs=(P(split, None), P(("groups", "mp", "sub"), None), P("groups")),
        check_vma=False,
    )
```

```python
import functools

import jax
import jax.numpy as jnp
from jax import lax
from jax.experimental import pallas as pl
from jax.experimental.pallas import tpu as pltpu
from jax.sharding import PartitionSpec as P


LANES = 128


def whole(*shape_and_type):
    return jax.ShapeDtypeStruct(*shape_and_type)


def on_chip(x):
    return pltpu.with_memory_space_constraint(x, pltpu.VMEM)


def vmem_specs(count):
    return [pl.BlockSpec(memory_space=pltpu.VMEM)] * count


def score_kernel(capacity, emb_ref, w1_ref, w2_ref, owner_ref, query_ref, label_ref, sent_ref, slot_ref):
    rows = emb_ref.shape[0]
    halves = sent_ref.shape[1] // 4
    along = lax.broadcasted_iota(jnp.int32, (rows, rows), 1)
    down = lax.broadcasted_iota(jnp.int32, (rows, rows), 0)

    def column(row):
        return jnp.sum(jnp.where(along == down, row, 0), axis=1, keepdims=True)

    owner = owner_ref[...]
    owner_column = column(owner)
    earlier = jnp.where((owner_column == owner) & (along < down), 1, 0)
    slot = owner_column * capacity + jnp.sum(earlier, axis=1, keepdims=True)
    slot_ref[...] = slot
    mark = column(query_ref[...] + 1).astype(jnp.float32)
    label = column(label_ref[...]).astype(jnp.float32)

    pre_act = jnp.dot(emb_ref[...], w1_ref[...], preferred_element_type=jnp.float32)
    hidden = pre_act * jax.nn.sigmoid(pre_act)
    score = jnp.sum(hidden * w2_ref[...], axis=1, keepdims=True)

    lane = lax.broadcasted_iota(jnp.int32, (rows, LANES), 1)
    sent_ref[...] = jnp.zeros_like(sent_ref)
    for h in range(halves):
        here = slot == lane + h * LANES
        for place, value in enumerate((score, mark, label)):
            row = jnp.sum(jnp.where(here, value, 0.0), axis=0, keepdims=True)
            for target in range(sent_ref.shape[0]):
                sent_ref[target, place * halves + h : place * halves + h + 1, :] = row


def within_groups(x, capacity):
    lane = lax.broadcasted_iota(jnp.int32, x.shape, 1)
    out = [x]
    step = capacity // 2
    while step:
        upper = (lane & step) != 0
        spread = []
        for y in out:
            spread.append(jnp.where(upper, pltpu.roll(y, step, 1), y))
            spread.append(jnp.where(upper, y, pltpu.roll(y, LANES - step, 1)))
        out = spread
        step //= 2
    return out


def group_sum(x, capacity):
    lane = lax.broadcasted_iota(jnp.int32, x.shape, 1)
    step = capacity // 2
    while step:
        upper = (lane & step) != 0
        x = x + jnp.where(upper, pltpu.roll(x, step, 1), pltpu.roll(x, LANES - step, 1))
        step //= 2
    return x


def lambda_kernel(
    capacity, place_ref, got_ref, slot_ref, spread_ref, column_ref,
    score_by, mark_by, key_by, disc_by, row_scratch,
):
    sources = got_ref.shape[0]
    halves = got_ref.shape[1] // 4
    me = place_ref[0]
    rows = slot_ref.shape[0]
    source = lax.broadcasted_iota(jnp.int32, (sources, LANES), 0)
    lane = lax.broadcasted_iota(jnp.int32, (sources, LANES), 1)
    position = (source * capacity + lane % capacity).astype(jnp.float32)
    slots = float(sources * capacity)
    trip = 2 * sources
    lane_of_row = lax.broadcasted_iota(jnp.int32, (rows, LANES), 1)
    lambda_column = jnp.zeros((rows, 1), jnp.float32)
    for h in range(halves):
        half_score = got_ref[:, h, :] * 0.5
        mark = got_ref[:, halves + h, :]
        label = got_ref[:, 2 * halves + h, :]
        key = (label + 8.0 * mark) * slots - position
        counts = []
        for query in range(2):
            here = jnp.sum(jnp.where(mark == query + 1.0, 1.0, 0.0), axis=0, keepdims=True)
            counts.append(group_sum(jnp.broadcast_to(here, (8, LANES)), capacity)[:1, :])
        first, other = counts
        fellows = jnp.where(mark == 1.0, first, jnp.where(mark == 2.0, other, slots - first - other))
        above = jnp.where(mark == 1.0, other, jnp.where(mark == 2.0, 0.0, first + other))
        for ref, value in ((score_by, half_score), (mark_by, mark), (key_by, key)):
            for c, spread in enumerate(within_groups(value, capacity)):
                ref[c * sources : (c + 1) * sources, :] = spread

        def rank_step(step, sums):
            soft, ideal = sums
            base = pl.multiple_of(step * trip, trip)
            score_rows = score_by[pl.ds(base, trip), :]
            mark_rows = mark_by[pl.ds(base, trip), :]
            key_rows = key_by[pl.ds(base, trip), :]
            for r in range(trip):
                same = mark_rows[r : r + 1, :] == mark
                tilt = jnp.tanh(score_rows[r : r + 1, :] - half_score)
                soft = soft + jnp.where(same, tilt, 0.0)
                ideal = ideal + jnp.where(key_rows[r : r + 1, :] > key, 1.0, 0.0)
            return soft, ideal

        nothing = jnp.zeros((sources, LANES), jnp.float32)
        soft, ideal = lax.fori_loop(0, capacity * sources // trip, rank_step, (nothing, nothing))
        discount = 1.0 / jnp.log2(2.0 + (0.5 * (soft + fellows) - 0.5))
        gain = jnp.exp2(label) - 1.0
        term = gain / jnp.log2(2.0 + (ideal - above))
        for c, spread in enumerate(within_groups(discount, capacity)):
            disc_by[c * sources : (c + 1) * sources, :] = spread

        for place, value in enumerate((half_score, mark, gain, discount)):
            row_scratch[place * sources : (place + 1) * sources, :] = value
        own_score, own_mark, own_gain, own_disc = (
            row_scratch[pl.ds(place * sources + me, 1), :] for place in range(4)
        )
        ideal_sum = jnp.zeros((1, LANES), jnp.float32)
        for query in range(2):
            asked = query + 1.0
            per_lane = jnp.sum(jnp.where(mark == asked, term, 0.0), axis=0, keepdims=True)
            spread = group_sum(jnp.broadcast_to(per_lane, (8, LANES)), capacity)[:1, :]
            ideal_sum = jnp.where(own_mark == asked, spread, ideal_sum)
        inv_ideal = jnp.where(ideal_sum > 0.0, 1.0 / jnp.where(ideal_sum > 0.0, ideal_sum, 1.0), 0.0)

        total = jnp.zeros((sources, LANES), jnp.float32)
        for c in range(capacity):
            at = slice(c * sources, (c + 1) * sources)
            their_label = jnp.ceil(key_by[at, :] * (1.0 / slots)) - 8.0 * mark_by[at, :]
            their_gain = jnp.exp2(their_label) - 1.0
            gain_gap = own_gain - their_gain
            gap = 2.0 * (score_by[at, :] - own_score)
            pull = jax.nn.sigmoid(jnp.where(gain_gap > 0.0, gap, -gap))
            pair = -gain_gap * jnp.abs(own_disc - disc_by[at, :]) * pull
            total = total + jnp.where(mark_by[at, :] == own_mark, pair, 0.0)
        lambda_row = jnp.sum(total, axis=0, keepdims=True) * inv_ideal
        here = slot_ref[...] == lane_of_row + h * LANES
        lambda_column = lambda_column + jnp.sum(
            jnp.where(here, lambda_row, 0.0), axis=1, keepdims=True
        )

    column_ref[...] = lambda_column
    along = lax.broadcasted_iota(jnp.int32, (rows, rows), 1)
    down = lax.broadcasted_iota(jnp.int32, (rows, rows), 0)
    row = jnp.sum(jnp.where(along == down, lambda_column, 0.0), axis=0, keepdims=True)
    spread_ref[...] = jnp.broadcast_to(row[None], spread_ref.shape)


def slope_kernel(count, place_ref, w1_ref, w2_ref, *refs):
    emb_refs, out_ref = refs[:count], refs[count]
    units = w1_ref.shape[1]
    wide = out_ref.shape[2] - 2 * units
    mine = pl.ds(pl.multiple_of(place_ref[1] // 2 * wide, LANES), wide)
    for i, emb_ref in enumerate(emb_refs):
        pre_act = jnp.dot(emb_ref[...], w1_ref[...], preferred_element_type=jnp.float32)
        gate = jax.nn.sigmoid(pre_act)
        out_ref[i, :, units : 2 * units] = (pre_act * gate).astype(jnp.bfloat16)
        slope = gate * (1.0 + pre_act * (1.0 - gate))
        out_ref[i, :, :units] = (w2_ref[...] * slope).astype(jnp.bfloat16)
        out_ref[i, :, 2 * units :] = emb_ref[:, mine]


def slopes(place, w_first, w2_row, blocks, wide):
    rows, units = blocks[0].shape[0], w_first.shape[1]
    count = len(blocks)
    return pl.pallas_call(
        functools.partial(slope_kernel, count),
        out_shape=pltpu.VMEM((count, rows, 2 * units + wide), jnp.bfloat16),
        in_specs=[pl.BlockSpec(memory_space=pltpu.SMEM)] + vmem_specs(2 + count),
        out_specs=vmem_specs(1)[0],
        name="slopes",
    )(place, w_first, w2_row, *blocks)


def product_kernel(offsets, units, place_ref, lambda_ref, ready_ref, sent_ref):
    members, rows = lambda_ref.shape[0], lambda_ref.shape[2]
    my_member = place_ref[1] // 2
    along = lax.broadcasted_iota(jnp.int32, (rows, rows), 1)
    down = lax.broadcasted_iota(jnp.int32, (rows, rows), 0)
    total, second = None, None
    for i, offset in enumerate(offsets):
        block = lambda_ref[lax.rem(my_member + offset, members)]
        column = jnp.sum(jnp.where(along == down, block[:1], 0.0), axis=1, keepdims=True)
        part = (ready_ref[i, :, 2 * units :].astype(jnp.float32) * column).astype(jnp.bfloat16)
        product = lax.dot_general(
            part, ready_ref[i, :, :units], (((0,), (0,)), ((), ())),
            preferred_element_type=jnp.float32,
        )
        high = block.astype(jnp.bfloat16)
        low = (block - high.astype(jnp.float32)).astype(jnp.bfloat16)
        hidden = ready_ref[i, :, units : 2 * units]
        summed = jnp.dot(high, hidden, preferred_element_type=jnp.float32) + jnp.dot(
            low, hidden, preferred_element_type=jnp.float32
        )
        total = product if total is None else total + product
        second = summed if second is None else second + summed
    targets = sent_ref.shape[0]
    part_rows = total.shape[0] // targets
    columns = total.shape[1] // LANES
    rounded, second = total.astype(jnp.bfloat16), second.astype(jnp.bfloat16)
    for target in range(targets):
        for k in range(columns):
            at = slice(k * LANES, (k + 1) * LANES)
            sent_ref[target, k * part_rows : (k + 1) * part_rows, :] = rounded[
                target * part_rows : (target + 1) * part_rows, at
            ]
            row = part_rows * columns + k
            sent_ref[target, row : row + 1, :] = second[:1, at]


def sent_to_all(x, axis):
    count = lax.axis_size(axis)
    return lax.all_to_all(jnp.broadcast_to(x[None], (count, *x.shape)), axis, 0, 0, tiled=True)


def parity_blocks(block):
    lanes, subs = lax.axis_size("mp"), lax.axis_size("sub")

    def moved(x, by):
        return lax.ppermute(x, "mp", [(i, (i + by) % lanes) for i in range(lanes)])

    back, on = moved(block, 2), moved(block, -2)
    both_ways = [
        (i * subs + s, (i + (2 if s == 0 else -2)) % lanes * subs + s)
        for i in range(lanes)
        for s in range(subs)
    ]
    passed = jnp.where(lax.axis_index("sub") == 0, back, on)
    across = lax.ppermute(passed, ("mp", "sub"), both_ways)
    return back, on, across


def on_device(embeddings, owner_shard, query_local, labels, w_first, w_second):
    docs, lanes, subs = (lax.axis_size(axis) for axis in ("docs", "mp", "sub"))
    rows, width = embeddings.shape
    units = w_first.shape[1]
    capacity = 2 * rows // docs
    halves = docs * capacity // LANES
    w2_row = w_second.reshape(1, units)
    place = jnp.stack([lax.axis_index(axis) for axis in ("docs", "mp", "sub")]).astype(jnp.int32)
    back, on, across = parity_blocks(embeddings)
    members = lanes // 2
    sent, slot = pl.pallas_call(
        functools.partial(score_kernel, capacity),
        out_shape=(
            whole((docs, 4 * halves, LANES), jnp.float32),
            whole((rows, 1), jnp.int32),
        ),
        in_specs=vmem_specs(6),
        out_specs=tuple(vmem_specs(2)),
        name="score",
    )(
        embeddings, w_first, w2_row,
        owner_shard.reshape(1, rows), query_local.reshape(1, rows), labels.reshape(1, rows),
    )
    got = lax.all_to_all(sent, "docs", 0, 0, tiled=True)
    spread, lambda_column = pl.pallas_call(
        functools.partial(lambda_kernel, capacity),
        out_shape=(whole((members, 8, rows), jnp.float32), whole((rows, 1), jnp.float32)),
        in_specs=[pl.BlockSpec(memory_space=pltpu.SMEM)] + vmem_specs(2),
        out_specs=tuple(vmem_specs(2)),
        scratch_shapes=[pltpu.VMEM((docs * capacity, LANES), jnp.float32)] * 4
        + [pltpu.VMEM((4 * docs, LANES), jnp.float32)],
        name="lambdas",
    )(place, on_chip(got), slot)
    parities = [list(range(parity, lanes, 2)) for parity in range(2)]
    all_lambdas = lax.all_to_all(
        spread, "mp", 0, 0, axis_index_groups=parities, tiled=True
    )

    part_rows = width // (lanes * subs)
    targets = 2 * subs
    wide = targets * part_rows
    columns = units // LANES
    prepared = slopes(place, w_first, w2_row, [embeddings, back, on, across], wide)
    own_grad = lax.dot_general(
        prepared[0, :, :units], w_first, (((1,), (1,)), ((), ())), preferred_element_type=jnp.float32
    )
    emb_grad = (lambda_column * own_grad).astype(jnp.bfloat16)
    all_lambdas, emb_grad = lax.optimization_barrier((all_lambdas, emb_grad))
    offsets = (0, members - 1, 1, 2)
    sent = pl.pallas_call(
        functools.partial(product_kernel, offsets, units),
        out_shape=pltpu.VMEM((targets, (part_rows + 1) * columns, LANES), jnp.bfloat16),
        in_specs=[pl.BlockSpec(memory_space=pltpu.SMEM)] + vmem_specs(2),
        out_specs=vmem_specs(1)[0],
        name="product",
    )(place, on_chip(all_lambdas), on_chip(prepared))
    cells = [list(range(i, i + targets)) for i in range(0, lanes * subs, targets)]
    arrived = lax.all_to_all(
        sent, ("mp", "sub"), 0, 0, axis_index_groups=cells, tiled=True
    )
    line_sum = arrived.astype(jnp.float32).sum(axis=0).astype(jnp.bfloat16)
    first_rows = part_rows * columns
    tiles = line_sum[:first_rows].reshape(docs, first_rows // docs, LANES)
    second = jnp.broadcast_to(line_sum[first_rows:][None], (docs, columns, LANES))
    arrived = lax.all_to_all(jnp.concatenate([tiles, second], axis=1), "docs", 0, 0, tiled=True)
    shard_sum = arrived.astype(jnp.float32).sum(axis=0)
    spread = sent_to_all(shard_sum[: first_rows // docs].astype(jnp.bfloat16), "docs")
    shard_sum, spread = lax.optimization_barrier((shard_sum, spread))
    w_second_grad = shard_sum[first_rows // docs :].reshape(units)
    w_first_grad = (
        spread.reshape(columns, part_rows, LANES).transpose(1, 0, 2).reshape(part_rows, units)
    ).astype(jnp.float32)
    return (emb_grad, w_first_grad, w_second_grad)


def solution(mesh):
    split = ("groups", "docs", "mp", "sub")
    return jax.shard_map(
        on_device,
        mesh=mesh,
        in_specs=(P(split, None), P(split, None), P(split), P(split), P(), P()),
        out_specs=(P(split, None), P(("groups", "mp", "sub"), None), P("groups")),
        check_vma=False,
    )
```

```python
import functools

import jax
import jax.numpy as jnp
from jax import lax
from jax.experimental import pallas as pl
from jax.experimental.pallas import tpu as pltpu
from jax.sharding import PartitionSpec as P


LANES = 128


def whole(*shape_and_type):
    return jax.ShapeDtypeStruct(*shape_and_type)


def on_chip(x):
    return pltpu.with_memory_space_constraint(x, pltpu.VMEM)


def vmem_specs(count):
    return [pl.BlockSpec(memory_space=pltpu.VMEM)] * count


def score_kernel(capacity, emb_ref, w1_ref, w2_ref, owner_ref, query_ref, label_ref, sent_ref, slot_ref):
    rows = emb_ref.shape[0]
    halves = sent_ref.shape[1] // 4
    along = lax.broadcasted_iota(jnp.int32, (rows, rows), 1)
    down = lax.broadcasted_iota(jnp.int32, (rows, rows), 0)

    def column(row):
        return jnp.sum(jnp.where(along == down, row, 0), axis=1, keepdims=True)

    owner = owner_ref[...]
    owner_column = column(owner)
    earlier = jnp.where((owner_column == owner) & (along < down), 1, 0)
    slot = owner_column * capacity + jnp.sum(earlier, axis=1, keepdims=True)
    slot_ref[...] = slot
    mark = column(query_ref[...] + 1).astype(jnp.float32)
    label = column(label_ref[...]).astype(jnp.float32)

    pre_act = jnp.dot(emb_ref[...], w1_ref[...], preferred_element_type=jnp.float32)
    hidden = pre_act * jax.nn.sigmoid(pre_act)
    score = jnp.sum(hidden * w2_ref[...], axis=1, keepdims=True)

    lane = lax.broadcasted_iota(jnp.int32, (rows, LANES), 1)
    sent_ref[...] = jnp.zeros_like(sent_ref)
    for h in range(halves):
        here = slot == lane + h * LANES
        for place, value in enumerate((score, mark, label)):
            row = jnp.sum(jnp.where(here, value, 0.0), axis=0, keepdims=True)
            for target in range(sent_ref.shape[0]):
                sent_ref[target, place * halves + h : place * halves + h + 1, :] = row


def within_groups(x, capacity):
    lane = lax.broadcasted_iota(jnp.int32, x.shape, 1)
    out = [x]
    step = capacity // 2
    while step:
        upper = (lane & step) != 0
        spread = []
        for y in out:
            spread.append(jnp.where(upper, pltpu.roll(y, step, 1), y))
            spread.append(jnp.where(upper, y, pltpu.roll(y, LANES - step, 1)))
        out = spread
        step //= 2
    return out


def group_sum(x, capacity):
    lane = lax.broadcasted_iota(jnp.int32, x.shape, 1)
    step = capacity // 2
    while step:
        upper = (lane & step) != 0
        x = x + jnp.where(upper, pltpu.roll(x, step, 1), pltpu.roll(x, LANES - step, 1))
        step //= 2
    return x


def lambda_kernel(
    capacity, place_ref, got_ref, slot_ref, spread_ref, column_ref,
    score_by, mark_by, key_by, disc_by, row_scratch,
):
    sources = got_ref.shape[0]
    halves = got_ref.shape[1] // 4
    me = place_ref[0]
    rows = slot_ref.shape[0]
    source = lax.broadcasted_iota(jnp.int32, (sources, LANES), 0)
    lane = lax.broadcasted_iota(jnp.int32, (sources, LANES), 1)
    position = (source * capacity + lane % capacity).astype(jnp.float32)
    slots = float(sources * capacity)
    trip = 4 * sources
    lane_of_row = lax.broadcasted_iota(jnp.int32, (rows, LANES), 1)
    lambda_column = jnp.zeros((rows, 1), jnp.float32)
    for h in range(halves):
        half_score = got_ref[:, h, :] * 0.5
        mark = got_ref[:, halves + h, :]
        label = got_ref[:, 2 * halves + h, :]
        key = (label + 8.0 * mark) * slots - position
        counts = []
        for query in range(2):
            here = jnp.sum(jnp.where(mark == query + 1.0, 1.0, 0.0), axis=0, keepdims=True)
            counts.append(group_sum(jnp.broadcast_to(here, (8, LANES)), capacity)[:1, :])
        first, other = counts
        fellows = jnp.where(mark == 1.0, first, jnp.where(mark == 2.0, other, slots - first - other))
        above = jnp.where(mark == 1.0, other, jnp.where(mark == 2.0, 0.0, first + other))
        for ref, value in ((score_by, half_score), (mark_by, mark), (key_by, key)):
            for c, spread in enumerate(within_groups(value, capacity)):
                ref[c * sources : (c + 1) * sources, :] = spread

        def rank_step(step, sums):
            soft, ideal = sums
            base = pl.multiple_of(step * trip, trip)
            score_rows = score_by[pl.ds(base, trip), :]
            mark_rows = mark_by[pl.ds(base, trip), :]
            key_rows = key_by[pl.ds(base, trip), :]
            for r in range(trip):
                same = mark_rows[r : r + 1, :] == mark
                tilt = jnp.tanh(score_rows[r : r + 1, :] - half_score)
                soft = soft + jnp.where(same, tilt, 0.0)
                ideal = ideal + jnp.where(key_rows[r : r + 1, :] > key, 1.0, 0.0)
            return soft, ideal

        nothing = jnp.zeros((sources, LANES), jnp.float32)
        soft, ideal = lax.fori_loop(0, capacity * sources // trip, rank_step, (nothing, nothing))
        discount = 1.0 / jnp.log2(2.0 + (0.5 * (soft + fellows) - 0.5))
        gain = jnp.exp2(label) - 1.0
        term = gain / jnp.log2(2.0 + (ideal - above))
        for c, spread in enumerate(within_groups(discount, capacity)):
            disc_by[c * sources : (c + 1) * sources, :] = spread

        for place, value in enumerate((half_score, mark, gain, discount)):
            row_scratch[place * sources : (place + 1) * sources, :] = value
        own_score, own_mark, own_gain, own_disc = (
            row_scratch[pl.ds(place * sources + me, 1), :] for place in range(4)
        )
        ideal_sum = jnp.zeros((1, LANES), jnp.float32)
        for query in range(2):
            asked = query + 1.0
            per_lane = jnp.sum(jnp.where(mark == asked, term, 0.0), axis=0, keepdims=True)
            spread = group_sum(jnp.broadcast_to(per_lane, (8, LANES)), capacity)[:1, :]
            ideal_sum = jnp.where(own_mark == asked, spread, ideal_sum)
        inv_ideal = jnp.where(ideal_sum > 0.0, 1.0 / jnp.where(ideal_sum > 0.0, ideal_sum, 1.0), 0.0)

        total = jnp.zeros((sources, LANES), jnp.float32)
        for c in range(capacity):
            at = slice(c * sources, (c + 1) * sources)
            their_label = jnp.ceil(key_by[at, :] * (1.0 / slots)) - 8.0 * mark_by[at, :]
            their_gain = jnp.exp2(their_label) - 1.0
            gain_gap = own_gain - their_gain
            gap = 2.0 * (score_by[at, :] - own_score)
            pull = jax.nn.sigmoid(jnp.where(gain_gap > 0.0, gap, -gap))
            pair = -gain_gap * jnp.abs(own_disc - disc_by[at, :]) * pull
            total = total + jnp.where(mark_by[at, :] == own_mark, pair, 0.0)
        lambda_row = jnp.sum(total, axis=0, keepdims=True) * inv_ideal
        here = slot_ref[...] == lane_of_row + h * LANES
        lambda_column = lambda_column + jnp.sum(
            jnp.where(here, lambda_row, 0.0), axis=1, keepdims=True
        )

    column_ref[...] = lambda_column
    along = lax.broadcasted_iota(jnp.int32, (rows, rows), 1)
    down = lax.broadcasted_iota(jnp.int32, (rows, rows), 0)
    row = jnp.sum(jnp.where(along == down, lambda_column, 0.0), axis=0, keepdims=True)
    spread_ref[...] = jnp.broadcast_to(row[None], spread_ref.shape)


def slope_kernel(count, place_ref, w1_ref, w2_ref, *refs):
    emb_refs, out_ref = refs[:count], refs[count]
    units = w1_ref.shape[1]
    wide = out_ref.shape[2] - 2 * units
    mine = pl.ds(pl.multiple_of(place_ref[1] // 2 * wide, LANES), wide)
    for i, emb_ref in enumerate(emb_refs):
        pre_act = jnp.dot(emb_ref[...], w1_ref[...], preferred_element_type=jnp.float32)
        gate = jax.nn.sigmoid(pre_act)
        out_ref[i, :, units : 2 * units] = (pre_act * gate).astype(jnp.bfloat16)
        slope = gate * (1.0 + pre_act * (1.0 - gate))
        out_ref[i, :, :units] = (w2_ref[...] * slope).astype(jnp.bfloat16)
        out_ref[i, :, 2 * units :] = emb_ref[:, mine]


def slopes(place, w_first, w2_row, blocks, wide):
    rows, units = blocks[0].shape[0], w_first.shape[1]
    count = len(blocks)
    return pl.pallas_call(
        functools.partial(slope_kernel, count),
        out_shape=pltpu.VMEM((count, rows, 2 * units + wide), jnp.bfloat16),
        in_specs=[pl.BlockSpec(memory_space=pltpu.SMEM)] + vmem_specs(2 + count),
        out_specs=vmem_specs(1)[0],
        name="slopes",
    )(place, w_first, w2_row, *blocks)


def product_kernel(offsets, units, place_ref, lambda_ref, ready_ref, sent_ref):
    members, rows = lambda_ref.shape[0], lambda_ref.shape[2]
    my_member = place_ref[1] // 2
    along = lax.broadcasted_iota(jnp.int32, (rows, rows), 1)
    down = lax.broadcasted_iota(jnp.int32, (rows, rows), 0)
    total, second = None, None
    for i, offset in enumerate(offsets):
        block = lambda_ref[lax.rem(my_member + offset, members)]
        column = jnp.sum(jnp.where(along == down, block[:1], 0.0), axis=1, keepdims=True)
        part = (ready_ref[i, :, 2 * units :].astype(jnp.float32) * column).astype(jnp.bfloat16)
        product = lax.dot_general(
            part, ready_ref[i, :, :units], (((0,), (0,)), ((), ())),
            preferred_element_type=jnp.float32,
        )
        high = block.astype(jnp.bfloat16)
        low = (block - high.astype(jnp.float32)).astype(jnp.bfloat16)
        hidden = ready_ref[i, :, units : 2 * units]
        summed = jnp.dot(high, hidden, preferred_element_type=jnp.float32) + jnp.dot(
            low, hidden, preferred_element_type=jnp.float32
        )
        total = product if total is None else total + product
        second = summed if second is None else second + summed
    targets = sent_ref.shape[0]
    part_rows = total.shape[0] // targets
    columns = total.shape[1] // LANES
    rounded, second = total.astype(jnp.bfloat16), second.astype(jnp.bfloat16)
    for target in range(targets):
        for k in range(columns):
            at = slice(k * LANES, (k + 1) * LANES)
            sent_ref[target, k * part_rows : (k + 1) * part_rows, :] = rounded[
                target * part_rows : (target + 1) * part_rows, at
            ]
            row = part_rows * columns + k
            sent_ref[target, row : row + 1, :] = second[:1, at]


def sent_to_all(x, axis):
    count = lax.axis_size(axis)
    return lax.all_to_all(jnp.broadcast_to(x[None], (count, *x.shape)), axis, 0, 0, tiled=True)


def parity_blocks(block):
    lanes, subs = lax.axis_size("mp"), lax.axis_size("sub")

    def moved(x, by):
        return lax.ppermute(x, "mp", [(i, (i + by) % lanes) for i in range(lanes)])

    back, on = moved(block, 2), moved(block, -2)
    both_ways = [
        (i * subs + s, (i + (2 if s == 0 else -2)) % lanes * subs + s)
        for i in range(lanes)
        for s in range(subs)
    ]
    passed = jnp.where(lax.axis_index("sub") == 0, back, on)
    across = lax.ppermute(passed, ("mp", "sub"), both_ways)
    return back, on, across


def on_device(embeddings, owner_shard, query_local, labels, w_first, w_second):
    docs, lanes, subs = (lax.axis_size(axis) for axis in ("docs", "mp", "sub"))
    rows, width = embeddings.shape
    units = w_first.shape[1]
    capacity = 2 * rows // docs
    halves = docs * capacity // LANES
    w2_row = w_second.reshape(1, units)
    place = jnp.stack([lax.axis_index(axis) for axis in ("docs", "mp", "sub")]).astype(jnp.int32)
    back, on, across = parity_blocks(embeddings)
    members = lanes // 2
    sent, slot = pl.pallas_call(
        functools.partial(score_kernel, capacity),
        out_shape=(
            whole((docs, 4 * halves, LANES), jnp.float32),
            whole((rows, 1), jnp.int32),
        ),
        in_specs=vmem_specs(6),
        out_specs=tuple(vmem_specs(2)),
        name="score",
    )(
        embeddings, w_first, w2_row,
        owner_shard.reshape(1, rows), query_local.reshape(1, rows), labels.reshape(1, rows),
    )
    got = lax.all_to_all(sent, "docs", 0, 0, tiled=True)
    spread, lambda_column = pl.pallas_call(
        functools.partial(lambda_kernel, capacity),
        out_shape=(whole((members, 8, rows), jnp.float32), whole((rows, 1), jnp.float32)),
        in_specs=[pl.BlockSpec(memory_space=pltpu.SMEM)] + vmem_specs(2),
        out_specs=tuple(vmem_specs(2)),
        scratch_shapes=[pltpu.VMEM((docs * capacity, LANES), jnp.float32)] * 4
        + [pltpu.VMEM((4 * docs, LANES), jnp.float32)],
        name="lambdas",
    )(place, on_chip(got), slot)
    parities = [list(range(parity, lanes, 2)) for parity in range(2)]
    all_lambdas = lax.all_to_all(
        spread, "mp", 0, 0, axis_index_groups=parities, tiled=True
    )

    part_rows = width // (lanes * subs)
    targets = 2 * subs
    wide = targets * part_rows
    columns = units // LANES
    prepared = slopes(place, w_first, w2_row, [embeddings, back, on, across], wide)
    offsets = (0, members - 1, 1, 2)
    sent = pl.pallas_call(
        functools.partial(product_kernel, offsets, units),
        out_shape=pltpu.VMEM((targets, (part_rows + 1) * columns, LANES), jnp.bfloat16),
        in_specs=[pl.BlockSpec(memory_space=pltpu.SMEM)] + vmem_specs(2),
        out_specs=vmem_specs(1)[0],
        name="product",
    )(place, on_chip(all_lambdas), on_chip(prepared))
    cells = [list(range(i, i + targets)) for i in range(0, lanes * subs, targets)]
    arrived = lax.all_to_all(
        sent, ("mp", "sub"), 0, 0, axis_index_groups=cells, tiled=True
    )
    line_sum = arrived.astype(jnp.float32).sum(axis=0).astype(jnp.bfloat16)
    first_rows = part_rows * columns
    tiles = line_sum[:first_rows].reshape(docs, first_rows // docs, LANES)
    second = jnp.broadcast_to(line_sum[first_rows:][None], (docs, columns, LANES))
    arrived = lax.all_to_all(jnp.concatenate([tiles, second], axis=1), "docs", 0, 0, tiled=True)
    shard_sum = arrived.astype(jnp.float32).sum(axis=0)
    lambda_column, shard_sum = lax.optimization_barrier((lambda_column, shard_sum))
    own_grad = lax.dot_general(
        prepared[0, :, :units], w_first, (((1,), (1,)), ((), ())), preferred_element_type=jnp.float32
    )
    emb_grad = (lambda_column * own_grad).astype(jnp.bfloat16)
    w_second_grad = shard_sum[first_rows // docs :].reshape(units)
    spread = sent_to_all(shard_sum[: first_rows // docs].astype(jnp.bfloat16), "docs")
    w_first_grad = (
        spread.reshape(columns, part_rows, LANES).transpose(1, 0, 2).reshape(part_rows, units)
    ).astype(jnp.float32)
    return (emb_grad, w_first_grad, w_second_grad)


def solution(mesh):
    split = ("groups", "docs", "mp", "sub")
    return jax.shard_map(
        on_device,
        mesh=mesh,
        in_specs=(P(split, None), P(split, None), P(split), P(split), P(), P()),
        out_specs=(P(split, None), P(("groups", "mp", "sub"), None), P("groups")),
        check_vma=False,
    )
```
